256 devices in a mesh: gx: 8 (over x, core), gy: 4 (over y), gz: 8 (over z).
Axes of the slice: x: 4, y: 4, z: 8, core: 2. Of those that a mesh axis runs over, the one named last changes fastest.
Arguments:
- offset: float32 [3, 8, 8, 16, 1024], P(None, None, 'gx', 'gy', 'gz'), may hold values from 0.05 to 0.95, as said below
- velocity: float32 [3, 8, 8, 16, 1024], P(None, None, 'gx', 'gy', 'gz'), may hold values from -11 to 11
- occupancy: int32 [8, 16, 1024], P('gx', 'gy', 'gz'), may hold values from 1 to 8
- noise: bfloat16 [14, 8, 8, 8, 16, 1024], P(None, None, None, 'gx', 'gy', 'gz'), may hold values from -4 to 4
Outputs:
- interaction_push_per_bead: float32 [3, 8, 8, 16, 1024], P(None, None, 'gx', 'gy', 'gz')
- stress_matrix: float32 [3, 3], replicated
- thermal_level: float32 [1], replicated
The draws below stay inside these ranges and needn't reach their ends.
Inputs may be any that keep to these rules, and one draw needn't show every extreme that they name: `offset`: two beads of the grid are never closer than 0.1. `occupancy`: at most 8 beads a cell, in its first slots.
All inputs are finite; a program needn't handle non-finite values.
Results may differ from the reference program's by a relative error of at most 0.0003.
Values may be sent and summed in bfloat16 or wider, within the bound.
No kernel may reach another device: no remote copies, remote signals or barrier semaphores. Data moves between devices by JAX's collectives and lax.ppermute only.
A program may use at most 64 MiB of HBM per device.

```python
from functools import partial
import jax
import jax.numpy as jnp
from jax import lax

P_SIZE = 8
NX = 8
NY = 16
NZ = 1024


def draw_offset(key, part):
    shape = (3, P_SIZE, NX, NY, NZ)
    comp = lax.broadcasted_iota(jnp.int32, shape, 0)
    slot = lax.broadcasted_iota(jnp.int32, shape, 1)
    half = (slot // 2 ** comp % 2).astype(jnp.float32)
    base = jax.random.uniform(key, shape, jnp.float32)
    random_kick = 0.05 + 0.4 * base
    return 0.5 * half + random_kick


def draw_velocity(key, part):
    shape = (3, P_SIZE, NX, NY, NZ)
    xpos = lax.broadcasted_iota(jnp.int32, shape, 2).astype(jnp.float32)
    ypos = lax.broadcasted_iota(jnp.int32, shape, 3).astype(jnp.float32)
    zpos = lax.broadcasted_iota(jnp.int32, shape, 4).astype(jnp.float32)
    heat = 0.25 * (1.0 + 2.0 * xpos / NX) * (1.0 + 2.0 * ypos / NY) * (1.0 + 2.0 * zpos / NZ)
    raw = jax.random.truncated_normal(key, -4.0, 4.0, shape, jnp.float32)
    return raw * jnp.sqrt(heat)


def with_ends(result, key, low, high):
    longest = result.shape.index(max(result.shape))
    spots = []
    for shift in (0, 1):
        where = [jax.random.randint(jax.random.fold_in(key, axis), (), 0, length) for axis, length in enumerate(result.shape)]
        where[longest] = (where[longest] + shift) % result.shape[longest]
        spots.append(tuple(where))
    return result.at[spots[0]].set(low).at[spots[1]].set(high)


def block_scale(own_key, extent, split, low, high):
    def one(position, blocks):
        draws = jax.random.uniform(jax.random.fold_in(jax.random.fold_in(own_key, 6), position), (blocks,), jnp.float32, low / len(split), high / len(split))
        return jnp.repeat(jnp.exp(draws), extent[position] // blocks).reshape((-1,) + (1,) * (len(extent) - position - 1))

    level = one(*split[0])
    for cut in split[1:]:
        level = level * one(*cut)
    return level


def bell_draw(stream_key, shape, scale, reach, pieces=(), held_as=jnp.bfloat16):
    entries = scale * jax.random.normal(stream_key, shape, jnp.float32)
    if pieces:
        entries = entries * block_scale(stream_key, shape, pieces, -0.22, 0.18)
    return jnp.clip(entries, -reach, reach).astype(held_as)


def setup_inputs(seed: int = 0) -> dict:
    seeds = jax.random.split(jax.random.key(seed), 5)
    return {
        "offset": draw_offset(jax.random.fold_in(seeds[4], 71), 0),
        "velocity": draw_velocity(jax.random.fold_in(seeds[4], 71), 0),
        "occupancy": with_ends(jax.random.randint(seeds[2], (NX, NY, NZ), 1, P_SIZE + 1), jax.random.fold_in(seeds[2], 1), 1, P_SIZE).astype(jnp.int32),
        "noise": bell_draw(seeds[3], (14, P_SIZE, P_SIZE, NX, NY, NZ), 1.0, 4.0, ((3, 8), (4, 4), (5, 8))),
    }


REPULSION = 25.0
FRICTION = 4.5
NOISE_SCALE = 15.0
forward_shifts = [(1, 0, 0), (-1, 1, 0), (0, 1, 0), (1, 1, 0)] + [(dx, dy, 1) for dy in (-1, 0, 1) for dx in (-1, 0, 1)]

def outer_total(left, right):
    product = left[:, None] * right[None, :]
    return lax.optimization_barrier(jnp.sum(product.reshape(3, 3, -1), axis=2))

def pair_tile(own, other, theta, shift_vec, identical_couple):
    extra = (1,) * (own.ndim - 2)
    slots = own.shape[1]
    dvec = jnp.array(shift_vec, dtype=jnp.float32).reshape((3, 1, 1) + extra)
    sep = own[0:3, :, None] - other[0:3, None, :] - dvec
    rel_vel = own[3:6, :, None] - other[3:6, None, :]
    live = own[6][:, None] * other[6][None, :]
    dist2 = lax.optimization_barrier(jnp.sum(sep * sep, axis=0))
    if identical_couple:
        same = (lax.broadcasted_iota(jnp.int32, (slots, slots), 0) == lax.broadcasted_iota(jnp.int32, (slots, slots), 1)).astype(jnp.float32).reshape((slots, slots) + extra)
        dist2 = dist2 + same
        live = live * (1.0 - same)
    dist = jnp.sqrt(dist2)
    weight = jnp.maximum(1.0 - dist, 0.0)
    unit = sep / dist
    closing_speed = lax.optimization_barrier(jnp.sum(unit * rel_vel, axis=0))
    force_magnitude = live * weight * (REPULSION - FRICTION * weight * closing_speed + NOISE_SCALE * theta)
    force = force_magnitude * unit
    clausius_moment = outer_total(sep, force)
    return (force, clausius_moment)

def plane_forces(args, shift_vec, identical_couple):
    own, other, theta = args
    force, clausius_moment = pair_tile(own, other, theta, shift_vec, identical_couple)
    return (lax.optimization_barrier(jnp.sum(force, axis=2)), lax.optimization_barrier(jnp.sum(force, axis=1)), clausius_moment)

def reference(offset, velocity, occupancy, noise):
    slots = offset.shape[1]
    live = (lax.broadcasted_iota(jnp.int32, (slots,) + occupancy.shape, 0) < occupancy[None]).astype(jnp.float32)
    pack = jnp.concatenate([offset, velocity, live[None]], axis=0)
    own_planes = jnp.moveaxis(pack, 2, 0)
    theta0 = noise[0].astype(jnp.float32)
    theta0 = (theta0 + jnp.swapaxes(theta0, 0, 1)) * 0.7071067811865476
    acting_upon_itself, unused, vir_self = lax.map(partial(plane_forces, shift_vec=(0, 0, 0), identical_couple=True), (own_planes, own_planes, jnp.moveaxis(theta0, 2, 0)))
    interaction_push_per_bead = jnp.moveaxis(acting_upon_itself, 0, 2)
    clausius_moment = 0.5 * lax.optimization_barrier(jnp.sum(vir_self, axis=0))
    for index, shift_vec in enumerate(forward_shifts):
        dx, dy, dz = shift_vec
        other = jnp.roll(pack, (-dx, -dy, -dz), axis=(2, 3, 4))
        theta = noise[index + 1].astype(jnp.float32)
        on_own, force_on_partner, vir = lax.map(partial(plane_forces, shift_vec=shift_vec, identical_couple=False), (own_planes, jnp.moveaxis(other, 2, 0), jnp.moveaxis(theta, 2, 0)))
        interaction_push_per_bead = interaction_push_per_bead + jnp.moveaxis(on_own, 0, 2)
        interaction_push_per_bead = interaction_push_per_bead - jnp.roll(jnp.moveaxis(force_on_partner, 0, 2), (dx, dy, dz), axis=(2, 3, 4))
        clausius_moment = clausius_moment + lax.optimization_barrier(jnp.sum(vir, axis=0))
    motion_work_sum = outer_total(velocity * live[None], velocity)
    couple_tally = jnp.sum(live)
    stress_matrix = (motion_work_sum + clausius_moment) / (NX * NY * NZ)
    thermal_level = jnp.reshape((motion_work_sum[0, 0] + motion_work_sum[1, 1] + motion_work_sum[2, 2]) / (3.0 * couple_tally - 3.0), (1,))
    return (interaction_push_per_bead, stress_matrix, thermal_level)
```

```python
import jax
import jax.numpy as jnp
from jax import lax
from jax.experimental import pallas as pl
from jax.experimental.pallas import tpu as pltpu
from jax.sharding import PartitionSpec as P

AXES = ("gx", "gy", "gz")
ROWS = 4
LANES = 128
SLOTS = 8
FAR = 100.0
NOISE_SCALE = 15.0
REST = 25.0 / 15.0
DRAG = 4.5 / 15.0
HALF_ROOT = 0.7071067811865476


def tile_index(dx, dy, dz):
    if dz == 1:
        return 5 + (dy + 1) * 3 + (dx + 1)
    return {(0, 0): 0, (1, 0): 1, (-1, 1): 2, (0, 1): 3, (1, 1): 4}[(dx, dy)]


COLUMN_TILES = {
    0: [(0, 0), (1, 0), (-1, 1), (0, 1), (1, 1)],
    1: [(0, 0), (1, 0), (-1, 1), (0, 1), (1, 1)],
    -1: [(1, 0), (-1, 1), (0, 1), (1, 1)],
}
PRODUCTS = [(0, 0), (0, 1), (0, 2), (1, 1), (1, 2), (2, 2)]


def lane_iota():
    return lax.broadcasted_iota(jnp.int32, (SLOTS, LANES), 1)


def slot_iota():
    return lax.broadcasted_iota(jnp.int32, (SLOTS, LANES), 0)


def row_of(ref, *index):
    *lead, s = index
    return jnp.broadcast_to(ref[(*lead, pl.ds(s, 1), slice(None))], (SLOTS, LANES))


def pack_kernel(off_ref, vel_ref, occ_ref, v_ref, ownx_ref, z_ref):
    lane = lane_iota()
    slot = slot_iota()
    z = jnp.zeros((SLOTS, LANES), jnp.float32)
    for y in range(ROWS):
        live = slot < jnp.broadcast_to(occ_ref[pl.ds(y, 1), :], (SLOTS, LANES))
        for c in range(6):
            if c < 3:
                val = off_ref[c, pl.ds(y, SLOTS, stride=ROWS), :]
                if c == 0:
                    ownx_ref[y] = jnp.where(live, val, FAR)
                    val = jnp.where(live, val, -FAR)
            else:
                val = vel_ref[c - 3, pl.ds(y, SLOTS, stride=ROWS), :] * DRAG
            v_ref[y * 6 + c] = val
            at = (y + 1) * 6 + c
            z = jnp.where(lane == at, pltpu.roll(val, at, 1), z)
    z_ref[...] = z


def widen_kernel(v_ref, zr_ref, ym_ref, yp_ref, m_ref):
    lane = lane_iota()
    for c in range(6):
        m_ref[c] = ym_ref[c]
        m_ref[30 + c] = yp_ref[c]
        for y in range(ROWS):
            m_ref[(y + 1) * 6 + c] = v_ref[y * 6 + c]
    z = jnp.where(lane < 6, pltpu.roll(ym_ref[6], LANES - 24, 1), zr_ref[...])
    z = jnp.where((lane >= 30) & (lane < 36), pltpu.roll(yp_ref[6], 24, 1), z)
    m_ref[36] = z


def next_plane(m_ref, dx, up_ref):
    lane = lane_iota()
    z = m_ref[36]
    for row in range(6):
        for c in range(6):
            at = row * 6 + c
            val = pltpu.roll(m_ref[at], LANES - 1, 1)
            val = jnp.where(lane == LANES - 1, pltpu.roll(z, LANES - 1 - at, 1), val)
            if c == 2:
                val = val + 1.0
            up_ref[at] = val


def row_pairs(y, columns, own_ref, ownx_ref, th_ref, rl_refs, ru_refs, vir):
    slot = slot_iota()
    d = [[None] * 3 for _ in range(SLOTS)]
    for dx, level_ref, up_ref in columns:
        for dy, dz in COLUMN_TILES[dx]:
            k = tile_index(dx, dy, dz)
            src = up_ref if dz else level_ref
            base = (y + 1 + dy) * 6
            oth = [src[base + c] for c in range(6)]
            if dx:
                oth[0] = oth[0] + float(dx)
            if dy:
                oth[1] = oth[1] + float(dy)
            r = [None] * 3
            for s in range(SLOTS):
                if k == 0 and s == SLOTS - 1:
                    continue
                own = [row_of(ownx_ref, y, s)] + [row_of(own_ref, (y + 1) * 6 + c, s) for c in range(1, 6)]
                sep = [own[a] - oth[a] for a in range(3)]
                rel = [own[3 + a] - oth[3 + a] for a in range(3)]
                dist2 = sep[0] * sep[0] + sep[1] * sep[1] + sep[2] * sep[2]
                u = jnp.maximum(lax.rsqrt(dist2) - 1.0, 0.0)
                dot = sep[0] * rel[0] + sep[1] * rel[1] + sep[2] * rel[2]
                theta = th_ref[pl.ds(k * 256 + s * 32 + y, SLOTS, stride=ROWS), :]
                if k == 0:
                    theta = (theta + th_ref[pl.ds(s * ROWS + y, SLOTS, stride=32), :]) * HALF_ROOT
                fr = u * ((theta + REST) - u * dot)
                if k == 0:
                    fr = jnp.where(slot > s, fr, 0.0)
                for a in range(3):
                    f = fr * sep[a]
                    d[s][a] = f if d[s][a] is None else d[s][a] + f
                    r[a] = f if r[a] is None else r[a] + f
            ref = (ru_refs if dz else rl_refs)[dx]
            at = (y + 1 + dy) * 3
            for a in range(3):
                ref[at + a] = ref[at + a] + r[a]
            vir = [t - oth[a] * r[b] for t, (a, b) in zip(vir, PRODUCTS)]
    for s in range(SLOTS):
        own = [row_of(ownx_ref, y, s)] + [row_of(own_ref, (y + 1) * 6 + c, s) for c in range(1, 3)]
        vir = [t + own[a] * d[s][b] for t, (a, b) in zip(vir, PRODUCTS)]
    return d, vir


def settle(rl_ref, ru_ref, out_ref):
    lane = lane_iota()
    z = jnp.zeros((SLOTS, LANES), jnp.float32)
    for at in range(18):
        up = ru_ref[at]
        z = jnp.where(lane == at, pltpu.roll(up, at + 1, 1), z)
        out_ref[1 + at] = rl_ref[at] + jnp.where(lane == 0, 0.0, pltpu.roll(up, 1, 1))
    out_ref[0] = z
    out_ref[19] = z


def own_column_kernel(m_ref, ownx_ref, th_ref, d_ref, r_ref, acc_ref, up_ref, rl_ref, ru_ref):
    next_plane(m_ref, 0, up_ref)
    zero = jnp.zeros((18, SLOTS, LANES), jnp.float32)
    rl_ref[...] = zero
    ru_ref[...] = zero
    acc_ref[...] = jnp.zeros((16, SLOTS, LANES), jnp.float32)

    @pl.loop(0, ROWS)
    def _(y):
        vir = [acc_ref[i] for i in range(6)]
        d, vir = row_pairs(y, [(0, m_ref, up_ref)], m_ref, ownx_ref, th_ref, {0: rl_ref}, {0: ru_ref}, vir)
        for i in range(6):
            acc_ref[i] = vir[i]
        for s in range(SLOTS):
            for a in range(3):
                part = d[s][a]
                d_ref[y * 3 + a, pl.ds(s, 1), :] = jnp.sum(part, axis=0, keepdims=True)
        base = (y + 1) * 6
        live = jnp.where(m_ref[base] > -0.5 * FAR, 1.0, 0.0)
        vel = [m_ref[base + 3 + a] for a in range(3)]
        for i, (a, b) in enumerate(PRODUCTS):
            acc_ref[6 + i] = acc_ref[6 + i] + live * vel[a] * vel[b]
        acc_ref[12] = acc_ref[12] + live

    settle(rl_ref, ru_ref, r_ref)


def side_columns_kernel(
    m_ref, ownx_ref, th_ref, xm_ref, xp_ref, d0_ref, acc0_ref,
    d_ref, rm_ref, rp_ref, tally_ref,
    um_ref, up_ref, rlm_ref, rum_ref, rlp_ref, rup_ref, acc_ref,
):
    next_plane(xm_ref, -1, um_ref)
    next_plane(xp_ref, 1, up_ref)
    zero = jnp.zeros((18, SLOTS, LANES), jnp.float32)
    for ref in (rlm_ref, rum_ref, rlp_ref, rup_ref):
        ref[...] = zero
    acc_ref[...] = acc0_ref[...]

    @pl.loop(0, ROWS)
    def _(y):
        vir = [acc_ref[i] for i in range(6)]
        d, vir = row_pairs(
            y, [(1, xp_ref, up_ref), (-1, xm_ref, um_ref)], m_ref, ownx_ref, th_ref,
            {1: rlp_ref, -1: rlm_ref}, {1: rup_ref, -1: rum_ref}, vir,
        )
        for i in range(6):
            acc_ref[i] = vir[i]
        for s in range(SLOTS):
            for a in range(3):
                at = (y * 3 + a, pl.ds(s, 1), slice(None))
                d_ref[at] = d0_ref[at] + jnp.sum(d[s][a], axis=0, keepdims=True)

    settle(rlm_ref, rum_ref, rm_ref)
    settle(rlp_ref, rup_ref, rp_ref)
    lane = lax.broadcasted_iota(jnp.int32, (16, LANES), 1)
    line = lax.broadcasted_iota(jnp.int32, (16, LANES), 0)
    sums = jnp.sum(jnp.sum(acc_ref[...], axis=1), axis=1, keepdims=True)
    tally = jnp.sum(jnp.where(lane == line, sums, 0.0), axis=0, keepdims=True)
    tally_ref[...] = jnp.broadcast_to(tally, tally_ref.shape)


def last_plane_kernel(sz_ref, ym_ref, yp_ref, z_ref):
    lane = lane_iota()
    z = sz_ref[...]
    z = z + jnp.where((lane >= 3) & (lane < 6), pltpu.roll(ym_ref[...], LANES - 12, 1), 0.0)
    z = z + jnp.where((lane >= 12) & (lane < 15), pltpu.roll(yp_ref[...], 12, 1), 0.0)
    z_ref[...] = z


def finish_kernel(d_ref, s_ref, ym_ref, yp_ref, z_ref, f_ref):
    lane = lane_iota()
    for y in range(ROWS):
        for a in range(3):
            at = (y + 1) * 3 + a
            back = s_ref[1 + at]
            if y == 0:
                back = back + ym_ref[a]
            if y == ROWS - 1:
                back = back + yp_ref[1 + a]
            back = back + jnp.where(lane == 0, pltpu.roll(z_ref[...], LANES - at, 1), 0.0)
            f_ref[a, pl.ds(y, SLOTS, stride=ROWS), :] = NOISE_SCALE * (d_ref[y * 3 + a] - back)


def f32(*shape):
    return jax.ShapeDtypeStruct(shape, jnp.float32)


def vmem(*shape):
    return pltpu.VMEM(shape, jnp.float32)


def call(kernel, out_shape, scratch=()):
    return pl.pallas_call(kernel, out_shape=out_shape, scratch_shapes=list(scratch), name=kernel.__name__)


def shifted(shard, axis, by):
    count = lax.axis_size(axis)
    return lax.ppermute(shard, axis, [(i, (i + by) % count) for i in range(count)])


def per_device(offset, velocity, occupancy, noise):
    off = offset.reshape(3, SLOTS * ROWS, LANES)
    vel = velocity.reshape(3, SLOTS * ROWS, LANES)
    occ = occupancy.reshape(ROWS, LANES)
    theta = noise.reshape(14 * SLOTS * SLOTS * ROWS, LANES).astype(jnp.float32)
    v, ownx, z = call(pack_kernel, (f32(24, SLOTS, LANES), f32(ROWS, SLOTS, LANES), f32(SLOTS, LANES)))(off, vel, occ)
    zr = shifted(z, "gz", -1)
    from_ym = shifted(jnp.concatenate([v[18:24], zr[None]]), "gy", 1)
    from_yp = shifted(jnp.concatenate([v[0:6], zr[None]]), "gy", -1)
    m = call(widen_kernel, f32(37, SLOTS, LANES))(v, zr, from_ym, from_yp)
    from_xm = shifted(m, "gx", 1)
    from_xp = shifted(m, "gx", -1)
    tile = (SLOTS, LANES)
    d0, r0, acc0 = call(
        own_column_kernel,
        (f32(12, *tile), f32(20, *tile), f32(16, *tile)),
        [vmem(36, *tile), vmem(18, *tile), vmem(18, *tile)],
    )(m, ownx, theta)
    devices = lax.axis_size(AXES)
    d, rm, rp, tally = call(
        side_columns_kernel,
        (f32(12, *tile), f32(20, *tile), f32(20, *tile), f32(devices, LANES)),
        [vmem(36, *tile)] * 2 + [vmem(18, *tile)] * 4 + [vmem(16, *tile)],
    )(m, ownx, theta, from_xm, from_xp, d0, acc0)
    s = r0 + shifted(rp, "gx", 1) + shifted(rm, "gx", -1)
    back_ym = shifted(s[16:20], "gy", 1)
    back_yp = shifted(s[0:4], "gy", -1)
    home = call(last_plane_kernel, f32(*tile))(s[0], back_ym[3], back_yp[0])
    arrived = shifted(home, "gz", 1)
    force = call(finish_kernel, f32(3, SLOTS * ROWS, LANES))(d, s, back_ym, back_yp, arrived)
    tallies = lax.all_to_all(tally, AXES, 0, 0, tiled=True)
    total = jnp.sum(tallies, axis=0)
    virial = NOISE_SCALE * total[0:6]
    kinetic = total[6:12] / (DRAG * DRAG)
    count = total[12]
    cells = ROWS * LANES * devices
    stress = (kinetic + virial) / cells
    order = [PRODUCTS.index((min(a, b), max(a, b))) for a in range(3) for b in range(3)]
    stress_matrix = jnp.stack([stress[i] for i in order]).reshape(3, 3)
    thermal_level = jnp.reshape((kinetic[0] + kinetic[3] + kinetic[5]) / (3.0 * count - 3.0), (1,))
    return force.reshape(offset.shape), stress_matrix, thermal_level


def solution(mesh):
    spec = P(None, None, *AXES)
    return jax.shard_map(
        per_device,
        mesh=mesh,
        in_specs=(spec, spec, P(*AXES), P(None, None, None, *AXES)),
        out_specs=(spec, P(), P()),
        check_vma=False,
    )
```

```python
import functools

import jax
import jax.numpy as jnp
from jax import lax
from jax.experimental import pallas as pl
from jax.experimental.pallas import tpu as pltpu
from jax.sharding import PartitionSpec as P

AXES = ("gx", "gy", "gz")
ROWS = 4
LANES = 128
SLOTS = 8
FAR = 100.0
NOISE_SCALE = 15.0
REST = 25.0 / 15.0
DRAG = 4.5 / 15.0
HALF_ROOT = 0.7071067811865476


def tile_index(dx, dy, dz):
    if dz == 1:
        return 5 + (dy + 1) * 3 + (dx + 1)
    return {(0, 0): 0, (1, 0): 1, (-1, 1): 2, (0, 1): 3, (1, 1): 4}[(dx, dy)]


COLUMN_TILES = {
    0: [(0, 0), (1, 0), (-1, 1), (0, 1), (1, 1)],
    1: [(0, 0), (1, 0), (-1, 1), (0, 1), (1, 1)],
    -1: [(1, 0), (-1, 1), (0, 1), (1, 1)],
}
PRODUCTS = [(0, 0), (0, 1), (0, 2), (1, 1), (1, 2), (2, 2)]


def lane_iota():
    return lax.broadcasted_iota(jnp.int32, (SLOTS, LANES), 1)


def slot_iota():
    return lax.broadcasted_iota(jnp.int32, (SLOTS, LANES), 0)


def row_of(ref, *index):
    *lead, s = index
    return jnp.broadcast_to(ref[(*lead, pl.ds(s, 1), slice(None))], (SLOTS, LANES))


def pack_kernel(off_ref, vel_ref, occ_ref, v_ref, ownx_ref, z_ref):
    lane = lane_iota()
    slot = slot_iota()
    z = jnp.zeros((SLOTS, LANES), jnp.float32)
    for y in range(ROWS):
        live = slot < jnp.broadcast_to(occ_ref[pl.ds(y, 1), :], (SLOTS, LANES))
        for c in range(6):
            if c < 3:
                val = off_ref[c, pl.ds(y, SLOTS, stride=ROWS), :]
                if c == 0:
                    ownx_ref[y] = jnp.where(live, val, FAR)
                    val = jnp.where(live, val, -FAR)
            else:
                val = vel_ref[c - 3, pl.ds(y, SLOTS, stride=ROWS), :] * DRAG
            v_ref[y * 6 + c] = val
            at = (y + 1) * 6 + c
            z = jnp.where(lane == at, pltpu.roll(val, at, 1), z)
    z_ref[...] = z


def convert_kernel(noise_ref, th_ref, ready_ref):
    ready_ref[...] = jnp.zeros_like(ready_ref)

    @pl.loop(0, th_ref.shape[0] // 256)
    def _(i):
        at = pl.ds(pl.multiple_of(i * 256, 256), 256)
        th_ref[at, :] = noise_ref[at, :].astype(jnp.float32)


def widen_kernel(v_ref, zr_ref, ym_ref, yp_ref, m_ref):
    lane = lane_iota()
    for c in range(6):
        m_ref[c] = ym_ref[c]
        m_ref[30 + c] = yp_ref[c]
        for y in range(ROWS):
            m_ref[(y + 1) * 6 + c] = v_ref[y * 6 + c]
    z = jnp.where(lane < 6, pltpu.roll(ym_ref[6], LANES - 24, 1), zr_ref[...])
    z = jnp.where((lane >= 30) & (lane < 36), pltpu.roll(yp_ref[6], 24, 1), z)
    m_ref[36] = z


def next_plane(m_ref, dx, up_ref):
    lane = lane_iota()
    z = m_ref[36]
    for row in range(6):
        for c in range(6):
            at = row * 6 + c
            val = pltpu.roll(m_ref[at], LANES - 1, 1)
            val = jnp.where(lane == LANES - 1, pltpu.roll(z, LANES - 1 - at, 1), val)
            if c == 2:
                val = val + 1.0
            up_ref[at] = val


def row_pairs(y, columns, own_ref, ownx_ref, th_ref, rl_refs, ru_refs, vir):
    slot = slot_iota()
    d = [[None] * 3 for _ in range(SLOTS)]
    for dx, level_ref, up_ref in columns:
        for dy, dz in COLUMN_TILES[dx]:
            k = tile_index(dx, dy, dz)
            src = up_ref if dz else level_ref
            base = (y + 1 + dy) * 6
            oth = [src[base + c] for c in range(6)]
            if dx:
                oth[0] = oth[0] + float(dx)
            if dy:
                oth[1] = oth[1] + float(dy)
            r = [None] * 3
            for s in range(SLOTS):
                if k == 0 and s == SLOTS - 1:
                    continue
                own = [row_of(ownx_ref, y, s)] + [row_of(own_ref, (y + 1) * 6 + c, s) for c in range(1, 6)]
                sep = [own[a] - oth[a] for a in range(3)]
                rel = [own[3 + a] - oth[3 + a] for a in range(3)]
                dist2 = sep[0] * sep[0] + sep[1] * sep[1] + sep[2] * sep[2]
                u = jnp.maximum(lax.rsqrt(dist2) - 1.0, 0.0)
                dot = sep[0] * rel[0] + sep[1] * rel[1] + sep[2] * rel[2]
                theta = th_ref[pl.ds(k * 256 + s * 32 + y, SLOTS, stride=ROWS), :]
                if k == 0:
                    theta = (theta + th_ref[pl.ds(s * ROWS + y, SLOTS, stride=32), :]) * HALF_ROOT
                fr = u * ((theta + REST) - u * dot)
                if k == 0:
                    fr = jnp.where(slot > s, fr, 0.0)
                for a in range(3):
                    f = fr * sep[a]
                    d[s][a] = f if d[s][a] is None else d[s][a] + f
                    r[a] = f if r[a] is None else r[a] + f
            ref = (ru_refs if dz else rl_refs)[dx]
            at = (y + 1 + dy) * 3
            for a in range(3):
                ref[at + a] = ref[at + a] + r[a]
            vir = [t - oth[a] * r[b] for t, (a, b) in zip(vir, PRODUCTS)]
    for s in range(SLOTS):
        own = [row_of(ownx_ref, y, s)] + [row_of(own_ref, (y + 1) * 6 + c, s) for c in range(1, 3)]
        vir = [t + own[a] * d[s][b] for t, (a, b) in zip(vir, PRODUCTS)]
    return d, vir


def settle(rl_ref, ru_ref, out_ref):
    lane = lane_iota()
    z = jnp.zeros((SLOTS, LANES), jnp.float32)
    for at in range(18):
        up = ru_ref[at]
        z = jnp.where(lane == at, pltpu.roll(up, at + 1, 1), z)
        out_ref[1 + at] = rl_ref[at] + jnp.where(lane == 0, 0.0, pltpu.roll(up, 1, 1))
    out_ref[0] = z
    out_ref[19] = z


def own_column_kernel(m_ref, ownx_ref, th_ref, d_ref, r_ref, acc_ref, up_ref, rl_ref, ru_ref):
    next_plane(m_ref, 0, up_ref)
    zero = jnp.zeros((18, SLOTS, LANES), jnp.float32)
    rl_ref[...] = zero
    ru_ref[...] = zero
    acc_ref[...] = jnp.zeros((16, SLOTS, LANES), jnp.float32)

    @pl.loop(0, ROWS)
    def _(y):
        vir = [acc_ref[i] for i in range(6)]
        d, vir = row_pairs(y, [(0, m_ref, up_ref)], m_ref, ownx_ref, th_ref, {0: rl_ref}, {0: ru_ref}, vir)
        for i in range(6):
            acc_ref[i] = vir[i]
        for s in range(SLOTS):
            for a in range(3):
                part = d[s][a]
                d_ref[y * 3 + a, pl.ds(s, 1), :] = jnp.sum(part, axis=0, keepdims=True)
        base = (y + 1) * 6
        live = jnp.where(m_ref[base] > -0.5 * FAR, 1.0, 0.0)
        vel = [m_ref[base + 3 + a] for a in range(3)]
        for i, (a, b) in enumerate(PRODUCTS):
            acc_ref[6 + i] = acc_ref[6 + i] + live * vel[a] * vel[b]
        acc_ref[12] = acc_ref[12] + live

    settle(rl_ref, ru_ref, r_ref)


def side_columns_kernel(
    m_ref, ownx_ref, th_ref, xm_ref, xp_ref, d0_ref, acc0_ref,
    d_ref, rm_ref, rp_ref, tally_ref,
    um_ref, up_ref, rlm_ref, rum_ref, rlp_ref, rup_ref, acc_ref,
):
    next_plane(xm_ref, -1, um_ref)
    next_plane(xp_ref, 1, up_ref)
    zero = jnp.zeros((18, SLOTS, LANES), jnp.float32)
    for ref in (rlm_ref, rum_ref, rlp_ref, rup_ref):
        ref[...] = zero
    acc_ref[...] = acc0_ref[...]

    @pl.loop(0, ROWS)
    def _(y):
        vir = [acc_ref[i] for i in range(6)]
        d, vir = row_pairs(
            y, [(1, xp_ref, up_ref), (-1, xm_ref, um_ref)], m_ref, ownx_ref, th_ref,
            {1: rlp_ref, -1: rlm_ref}, {1: rup_ref, -1: rum_ref}, vir,
        )
        for i in range(6):
            acc_ref[i] = vir[i]
        for s in range(SLOTS):
            for a in range(3):
                at = (y * 3 + a, pl.ds(s, 1), slice(None))
                d_ref[at] = d0_ref[at] + jnp.sum(d[s][a], axis=0, keepdims=True)

    settle(rlm_ref, rum_ref, rm_ref)
    settle(rlp_ref, rup_ref, rp_ref)
    acc = [acc_ref[i] for i in range(13)]
    sums = [NOISE_SCALE * acc[i] + acc[6 + i] * (1.0 / (DRAG * DRAG)) for i in range(6)]
    lines = [sums[PRODUCTS.index((min(a, b), max(a, b)))] for a in range(3) for b in range(3)]
    lines += [(acc[6] + acc[9] + acc[11]) * (1.0 / (DRAG * DRAG)), acc[12]]
    lane = lax.broadcasted_iota(jnp.int32, (16, LANES), 1)
    line = lax.broadcasted_iota(jnp.int32, (16, LANES), 0)
    lines = [jnp.sum(x, axis=0, keepdims=True) for x in lines]
    held = jnp.concatenate(lines + [jnp.zeros((16 - len(lines), LANES), jnp.float32)], axis=0)
    held = jnp.where(lane == line, jnp.sum(held, axis=1, keepdims=True), 0.0)
    tally = jnp.sum(held, axis=0, keepdims=True)
    tally_ref[...] = jnp.broadcast_to(tally, tally_ref.shape)


def last_plane_kernel(s_ref, ym_ref, yp_ref, z_ref):
    lane = lane_iota()
    z = s_ref[0]
    z = z + jnp.where((lane >= 3) & (lane < 6), pltpu.roll(ym_ref[3], LANES - 12, 1), 0.0)
    z = z + jnp.where((lane >= 12) & (lane < 15), pltpu.roll(yp_ref[0], 12, 1), 0.0)
    z_ref[...] = z


def finish_kernel(d_ref, s_ref, ym_ref, yp_ref, z_ref, f_ref):
    lane = lane_iota()
    for y in range(ROWS):
        for a in range(3):
            at = (y + 1) * 3 + a
            back = s_ref[1 + at]
            if y == 0:
                back = back + ym_ref[a]
            if y == ROWS - 1:
                back = back + yp_ref[1 + a]
            back = back + jnp.where(lane == 0, pltpu.roll(z_ref[...], LANES - at, 1), 0.0)
            f_ref[a, pl.ds(y, SLOTS, stride=ROWS), :] = NOISE_SCALE * (d_ref[y * 3 + a] - back)


def report_kernel(cells, tallies_ref, stress_ref, level_ref):
    total = jnp.broadcast_to(jnp.sum(tallies_ref[...], axis=0, keepdims=True), (SLOTS, LANES))
    slot = slot_iota()
    stress = jnp.where(slot == 1, pltpu.roll(total, LANES - 3, 1), total)
    stress = jnp.where(slot == 2, pltpu.roll(total, LANES - 6, 1), stress) * (1.0 / cells)
    stress_ref[...] = stress[0:3, 0:3]
    level = pltpu.roll(total, LANES - 9, 1) / (3.0 * pltpu.roll(total, LANES - 10, 1) - 3.0)
    level_ref[...] = level[0:1, 0:1]


def f32(*shape):
    return pltpu.VMEM(shape, jnp.float32)


def vmem(*shape):
    return pltpu.VMEM(shape, jnp.float32)


def call(kernel, out_shape, scratch=(), hold=True):
    space = pl.BlockSpec(memory_space=pltpu.VMEM)

    def run(*args):
        if hold:
            args = [pltpu.with_memory_space_constraint(a, pltpu.VMEM) for a in args]
        return pl.pallas_call(
            kernel,
            out_shape=out_shape,
            in_specs=[space for _ in args],
            out_specs=jax.tree.map(lambda _: space, out_shape),
            scratch_shapes=list(scratch),
            compiler_params=pltpu.CompilerParams(vmem_limit_bytes=16 << 20),
            name=getattr(kernel, "func", kernel).__name__,
        )(*args)

    return run


def shifted(shard, axis, by):
    count = lax.axis_size(axis)
    return lax.ppermute(shard, axis, [(i, (i + by) % count) for i in range(count)])


def per_device(offset, velocity, occupancy, noise):
    off = offset.reshape(3, SLOTS * ROWS, LANES)
    vel = velocity.reshape(3, SLOTS * ROWS, LANES)
    occ = occupancy.reshape(ROWS, LANES)
    tile = (SLOTS, LANES)
    lines = 14 * SLOTS * SLOTS * ROWS
    theta, ready = call(convert_kernel, (f32(lines, LANES), f32(*tile)), hold=False)(noise.reshape(lines, LANES))
    v, ownx, z = call(pack_kernel, (f32(24, *tile), f32(ROWS, *tile), f32(*tile)), hold=False)(off, vel, occ)
    zr, ready = lax.optimization_barrier((shifted(z, "gz", -1), ready))
    zr = zr + ready
    from_ym = shifted(jnp.concatenate([v[18:24], zr[None]]), "gy", 1)
    from_yp = shifted(jnp.concatenate([v[0:6], zr[None]]), "gy", -1)
    m = call(widen_kernel, f32(37, *tile))(v, zr, from_ym, from_yp)
    from_xm = shifted(m, "gx", 1)
    from_xp = shifted(m, "gx", -1)
    d0, r0, acc0 = call(
        own_column_kernel,
        (f32(12, *tile), f32(20, *tile), f32(16, *tile)),
        [vmem(36, *tile), vmem(18, *tile), vmem(18, *tile)],
    )(m, ownx, theta)
    devices = lax.axis_size(AXES)
    d, rm, rp, tally = call(
        side_columns_kernel,
        (f32(12, *tile), f32(20, *tile), f32(20, *tile), f32(devices, LANES)),
        [vmem(36, *tile)] * 2 + [vmem(18, *tile)] * 4 + [vmem(16, *tile)],
    )(m, ownx, theta, from_xm, from_xp, d0, acc0)
    s = r0 + shifted(rp, "gx", 1) + shifted(rm, "gx", -1)
    back_ym = shifted(s[16:20], "gy", 1)
    back_yp = shifted(s[0:4], "gy", -1)
    home = call(last_plane_kernel, f32(*tile))(s, back_ym, back_yp)
    arrived = shifted(home, "gz", 1)
    force_shape = jax.ShapeDtypeStruct((3, SLOTS * ROWS, LANES), jnp.float32)
    force = call(finish_kernel, force_shape)(d, s, back_ym, back_yp, arrived)
    tallies = lax.all_to_all(tally, AXES, 0, 0, tiled=True)
    stress, level = call(
        functools.partial(report_kernel, float(ROWS * LANES * devices)),
        (jax.ShapeDtypeStruct((3, 3), jnp.float32), jax.ShapeDtypeStruct((1, 1), jnp.float32)),
    )(tallies)
    return force.reshape(offset.shape), stress, level.reshape(1)


def solution(mesh):
    spec = P(None, None, *AXES)
    return jax.shard_map(
        per_device,
        mesh=mesh,
        in_specs=(spec, spec, P(*AXES), P(None, None, None, *AXES)),
        out_specs=(spec, P(), P()),
        check_vma=False,
    )
```

```python
import functools

import jax
import jax.numpy as jnp
from jax import lax
from jax.experimental import pallas as pl
from jax.experimental.pallas import tpu as pltpu
from jax.sharding import PartitionSpec as P

AXES = ("gx", "gy", "gz")
ROWS = 4
LANES = 128
SLOTS = 8
FAR = 100.0
NOISE_SCALE = 15.0
REST = 25.0 / 15.0
DRAG = 4.5 / 15.0
HALF_ROOT = 0.7071067811865476
BACK = 16


def tile_index(dx, dy, dz):
    if dz == 1:
        return 5 + (dy + 1) * 3 + (dx + 1)
    return {(0, 0): 0, (1, 0): 1, (-1, 1): 2, (0, 1): 3, (1, 1): 4}[(dx, dy)]


COLUMN_TILES = {
    0: [(0, 0), (1, 0), (-1, 1), (0, 1), (1, 1)],
    1: [(0, 0), (1, 0), (-1, 1), (0, 1), (1, 1)],
    -1: [(1, 0), (-1, 1), (0, 1), (1, 1)],
}
PRODUCTS = [(0, 0), (0, 1), (0, 2), (1, 1), (1, 2), (2, 2)]


def lane_iota():
    return lax.broadcasted_iota(jnp.int32, (SLOTS, LANES), 1)


def slot_iota():
    return lax.broadcasted_iota(jnp.int32, (SLOTS, LANES), 0)


def row_of(ref, *index):
    *lead, s = index
    return jnp.broadcast_to(ref[(*lead, pl.ds(s, 1), slice(None))], (SLOTS, LANES))


def pack_kernel(off_hbm, vel_hbm, occ_hbm, v_ref, ownx_ref, z_ref, off_ref, vel_ref, occ_ref, sems):
    copies = [
        pltpu.make_async_copy(src, dst, sems.at[i])
        for i, (src, dst) in enumerate([(off_hbm, off_ref), (vel_hbm, vel_ref), (occ_hbm, occ_ref)])
    ]
    for copy in copies:
        copy.start()
    for copy in copies:
        copy.wait()
    lane = lane_iota()
    slot = slot_iota()
    z = jnp.zeros((SLOTS, LANES), jnp.float32)
    for y in range(ROWS):
        live = slot < jnp.broadcast_to(occ_ref[pl.ds(y, 1), :], (SLOTS, LANES))
        for c in range(6):
            if c < 3:
                val = off_ref[c, pl.ds(y, SLOTS, stride=ROWS), :]
                if c == 0:
                    ownx_ref[y] = jnp.where(live, val, FAR)
                    val = jnp.where(live, val, -FAR)
            else:
                val = vel_ref[c - 3, pl.ds(y, SLOTS, stride=ROWS), :] * DRAG
            v_ref[y * 6 + c] = val
            at = (y + 1) * 6 + c
            z = jnp.where(lane == at, pltpu.roll(val, at, 1), z)
    z_ref[...] = z


def convert_kernel(noise_ref, th_ref):
    @pl.loop(0, th_ref.shape[0] // 256)
    def _(i):
        at = pl.ds(pl.multiple_of(i * 256, 256), 256)
        th_ref[at, :] = noise_ref[at, :].astype(jnp.float32)


def widen_kernel(v_ref, zr_ref, ym_ref, yp_ref, m_ref):
    lane = lane_iota()
    for c in range(6):
        m_ref[c] = ym_ref[c]
        m_ref[30 + c] = yp_ref[c]
        for y in range(ROWS):
            m_ref[(y + 1) * 6 + c] = v_ref[y * 6 + c]
    z = jnp.where(lane < 6, pltpu.roll(ym_ref[6], LANES - 24, 1), zr_ref[...])
    z = jnp.where((lane >= 30) & (lane < 36), pltpu.roll(yp_ref[6], 24, 1), z)
    m_ref[36] = z


def next_plane(m_ref, dx, up_ref):
    lane = lane_iota()
    z = m_ref[36]
    for row in range(6):
        for c in range(6):
            at = row * 6 + c
            val = pltpu.roll(m_ref[at], LANES - 1, 1)
            val = jnp.where(lane == LANES - 1, pltpu.roll(z, LANES - 1 - at, 1), val)
            if c == 2:
                val = val + 1.0
            up_ref[at] = val


def row_pairs(y, columns, own_ref, ownx_ref, th_ref, rl_refs, ru_refs, vir):
    slot = slot_iota()
    d = [[None] * 3 for _ in range(SLOTS)]
    for dx, level_ref, up_ref in columns:
        for dy, dz in COLUMN_TILES[dx]:
            k = tile_index(dx, dy, dz)
            src = up_ref if dz else level_ref
            base = (y + 1 + dy) * 6
            oth = [src[base + c] for c in range(6)]
            if dx:
                oth[0] = oth[0] + float(dx)
            if dy:
                oth[1] = oth[1] + float(dy)
            r = [None] * 3
            for s in range(SLOTS):
                if k == 0 and s == SLOTS - 1:
                    continue
                own = [row_of(ownx_ref, y, s)] + [row_of(own_ref, (y + 1) * 6 + c, s) for c in range(1, 6)]
                sep = [own[a] - oth[a] for a in range(3)]
                rel = [own[3 + a] - oth[3 + a] for a in range(3)]
                dist2 = sep[0] * sep[0] + sep[1] * sep[1] + sep[2] * sep[2]
                u = jnp.maximum(lax.rsqrt(dist2) - 1.0, 0.0)
                dot = sep[0] * rel[0] + sep[1] * rel[1] + sep[2] * rel[2]
                theta = th_ref[pl.ds(k * 256 + s * 32 + y, SLOTS, stride=ROWS), :]
                if k == 0:
                    theta = (theta + th_ref[pl.ds(s * ROWS + y, SLOTS, stride=32), :]) * HALF_ROOT
                fr = u * ((theta + REST) - u * dot)
                if k == 0:
                    fr = jnp.where(slot > s, fr, 0.0)
                for a in range(3):
                    f = fr * sep[a]
                    d[s][a] = f if d[s][a] is None else d[s][a] + f
                    r[a] = f if r[a] is None else r[a] + f
            ref = (ru_refs if dz else rl_refs)[dx]
            at = (y + 1 + dy) * 3
            for a in range(3):
                ref[at + a] = ref[at + a] + r[a]
            vir = [t - oth[a] * r[b] for t, (a, b) in zip(vir, PRODUCTS)]
    for s in range(SLOTS):
        own = [row_of(ownx_ref, y, s)] + [row_of(own_ref, (y + 1) * 6 + c, s) for c in range(1, 3)]
        vir = [t + own[a] * d[s][b] for t, (a, b) in zip(vir, PRODUCTS)]
    return d, vir


def settle(rl_ref, ru_ref, out_ref):
    lane = lane_iota()
    z = jnp.zeros((SLOTS, LANES), jnp.float32)
    for at in range(18):
        up = ru_ref[at]
        z = jnp.where(lane == at, pltpu.roll(up, at + 1, 1), z)
        out_ref[at] = rl_ref[at] + jnp.where(lane == 0, 0.0, pltpu.roll(up, 1, 1))
    return z


def send_past(z, sizes, at, dx, tally, rows_ref):
    lane = lax.broadcasted_iota(jnp.int32, (1, LANES), 1)
    column = (at[0] + (dx + sizes[0])) % sizes[0] * sizes[1]
    for dy, row, count, place in [(-1, 0, 1, 3), (0, 1, 4, 0), (1, 5, 1, 0)]:
        line = tally
        for t in range(SLOTS):
            to = BACK + t * 12 + place * 3
            moved = pltpu.roll(z[t : t + 1, :], (to - row * 3) % LANES, 1)
            line = jnp.where((lane >= to) & (lane < to + 3 * count), moved, line)
        dest = (column + (at[1] + (dy + sizes[1])) % sizes[1]) * sizes[2] + (at[2] + 1) % sizes[2]
        rows_ref[pl.ds(dest, 1), :] = line


def own_column_kernel(m_ref, ownx_ref, th_ref, d_ref, r_ref, z_ref, acc_ref, up_ref, rl_ref, ru_ref):
    next_plane(m_ref, 0, up_ref)
    zero = jnp.zeros((18, SLOTS, LANES), jnp.float32)
    rl_ref[...] = zero
    ru_ref[...] = zero
    acc_ref[...] = jnp.zeros((16, SLOTS, LANES), jnp.float32)

    @pl.loop(0, ROWS)
    def _(y):
        vir = [acc_ref[i] for i in range(6)]
        d, vir = row_pairs(y, [(0, m_ref, up_ref)], m_ref, ownx_ref, th_ref, {0: rl_ref}, {0: ru_ref}, vir)
        for i in range(6):
            acc_ref[i] = vir[i]
        for s in range(SLOTS):
            for a in range(3):
                part = d[s][a]
                d_ref[y * 3 + a, pl.ds(s, 1), :] = jnp.sum(part, axis=0, keepdims=True)
        base = (y + 1) * 6
        live = jnp.where(m_ref[base] > -0.5 * FAR, 1.0, 0.0)
        vel = [m_ref[base + 3 + a] for a in range(3)]
        for i, (a, b) in enumerate(PRODUCTS):
            acc_ref[6 + i] = acc_ref[6 + i] + live * vel[a] * vel[b]
        acc_ref[12] = acc_ref[12] + live

    z_ref[...] = settle(rl_ref, ru_ref, r_ref)


def side_columns_kernel(
    sizes, here_ref, m_ref, ownx_ref, th_ref, xm_ref, xp_ref, d0_ref, z0_ref, acc0_ref,
    d_ref, rm_ref, rp_ref, tally_ref,
    um_ref, up_ref, rlm_ref, rum_ref, rlp_ref, rup_ref, acc_ref,
):
    next_plane(xm_ref, -1, um_ref)
    next_plane(xp_ref, 1, up_ref)
    zero = jnp.zeros((18, SLOTS, LANES), jnp.float32)
    for ref in (rlm_ref, rum_ref, rlp_ref, rup_ref):
        ref[...] = zero
    acc_ref[...] = acc0_ref[...]

    @pl.loop(0, ROWS)
    def _(y):
        vir = [acc_ref[i] for i in range(6)]
        d, vir = row_pairs(
            y, [(1, xp_ref, up_ref), (-1, xm_ref, um_ref)], m_ref, ownx_ref, th_ref,
            {1: rlp_ref, -1: rlm_ref}, {1: rup_ref, -1: rum_ref}, vir,
        )
        for i in range(6):
            acc_ref[i] = vir[i]
        for s in range(SLOTS):
            for a in range(3):
                at = (y * 3 + a, pl.ds(s, 1), slice(None))
                d_ref[at] = d0_ref[at] + jnp.sum(d[s][a], axis=0, keepdims=True)

    planes = [settle(rlm_ref, rum_ref, rm_ref), z0_ref[...], settle(rlp_ref, rup_ref, rp_ref)]
    acc = [acc_ref[i] for i in range(13)]
    sums = [NOISE_SCALE * acc[i] + acc[6 + i] * (1.0 / (DRAG * DRAG)) for i in range(6)]
    lines = [sums[PRODUCTS.index((min(a, b), max(a, b)))] for a in range(3) for b in range(3)]
    lines += [(acc[6] + acc[9] + acc[11]) * (1.0 / (DRAG * DRAG)), acc[12]]
    lane = lax.broadcasted_iota(jnp.int32, (16, LANES), 1)
    line = lax.broadcasted_iota(jnp.int32, (16, LANES), 0)
    lines = [jnp.sum(x, axis=0, keepdims=True) for x in lines]
    held = jnp.concatenate(lines + [jnp.zeros((16 - len(lines), LANES), jnp.float32)], axis=0)
    held = jnp.where(lane == line, jnp.sum(held, axis=1, keepdims=True), 0.0)
    tally = jnp.sum(held, axis=0, keepdims=True)
    tally_ref[...] = jnp.broadcast_to(tally, tally_ref.shape)
    at = (here_ref[0] // (sizes[1] * sizes[2]), here_ref[0] // sizes[2] % sizes[1], here_ref[0] % sizes[2])
    for dx, z in zip((-1, 0, 1), planes):
        send_past(z, sizes, at, dx, tally, tally_ref)


def finish_kernel(cells, d_ref, s_ref, ym_ref, yp_ref, tallies_ref, f_ref, stress_ref, level_ref):
    lane = lane_iota()
    slot = slot_iota()
    total = jnp.broadcast_to(jnp.sum(tallies_ref[...], axis=0, keepdims=True), (SLOTS, LANES))
    stress = jnp.where(slot == 1, pltpu.roll(total, LANES - 3, 1), total)
    stress = jnp.where(slot == 2, pltpu.roll(total, LANES - 6, 1), stress) * (1.0 / cells)
    stress_ref[...] = stress[0:3, 0:3]
    level = pltpu.roll(total, LANES - 9, 1) / (3.0 * pltpu.roll(total, LANES - 10, 1) - 3.0)
    level_ref[...] = level[0:1, 0:1]
    z = pltpu.roll(total, LANES - BACK, 1)
    for t in range(1, SLOTS):
        z = jnp.where(slot == t, pltpu.roll(total, LANES - BACK - t * 12, 1), z)
    for y in range(ROWS):
        for a in range(3):
            at = (y + 1) * 3 + a
            back = s_ref[at]
            if y == 0:
                back = back + ym_ref[a]
            if y == ROWS - 1:
                back = back + yp_ref[a]
            back = back + jnp.where(lane == 0, pltpu.roll(z, (LANES - y * 3 - a) % LANES, 1), 0.0)
            f_ref[a, pl.ds(y, SLOTS, stride=ROWS), :] = NOISE_SCALE * (d_ref[y * 3 + a] - back)


def f32(*shape):
    return pltpu.VMEM(shape, jnp.float32)


def vmem(*shape):
    return pltpu.VMEM(shape, jnp.float32)


def call(kernel, out_shape, scratch=(), source=None, scalars=0):
    space = pl.BlockSpec(memory_space=pltpu.VMEM)

    def run(*args):
        specs = [pl.BlockSpec(memory_space=source or pltpu.VMEM) for _ in args]
        specs[:scalars] = [pl.BlockSpec(memory_space=pltpu.SMEM)] * scalars
        if source is not pltpu.VMEM:
            held = [pltpu.with_memory_space_constraint(a, source or pltpu.VMEM) for a in args[scalars:]]
            args = (*args[:scalars], *held)
        return pl.pallas_call(
            kernel,
            out_shape=out_shape,
            in_specs=specs,
            out_specs=jax.tree.map(lambda _: space, out_shape),
            scratch_shapes=list(scratch),
            compiler_params=pltpu.CompilerParams(vmem_limit_bytes=16 << 20),
            name=getattr(kernel, "func", kernel).__name__,
        )(*args)

    return run


def swapped(shard, axis, first):
    count = lax.axis_size(axis)
    pairs = [((first + i) % count, (first + i + 1) % count) for i in range(0, count, 2)]
    return lax.ppermute(shard, axis, pairs + [(j, i) for i, j in pairs])


def both_sides(low, high, axis):
    even = lax.axis_index(axis) % 2 == 0
    inner = swapped(jnp.where(even, high, low), axis, 0)
    outer = swapped(jnp.where(even, low, high), axis, 1)
    return jnp.where(even, outer, inner), jnp.where(even, inner, outer)


def shifted(shard, axis, by):
    count = lax.axis_size(axis)
    return lax.ppermute(shard, axis, [(i, (i + by) % count) for i in range(count)])


def per_device(offset, velocity, occupancy, noise):
    off = offset.reshape(3, SLOTS * ROWS, LANES)
    vel = velocity.reshape(3, SLOTS * ROWS, LANES)
    occ = occupancy.reshape(ROWS, LANES)
    tile = (SLOTS, LANES)
    lines = 14 * SLOTS * SLOTS * ROWS
    theta = call(convert_kernel, f32(lines, LANES), source=pltpu.VMEM)(noise.reshape(lines, LANES))
    v, ownx, z = call(
        pack_kernel,
        (f32(24, *tile), f32(ROWS, *tile), f32(*tile)),
        [vmem(*off.shape), vmem(*off.shape), pltpu.VMEM(occ.shape, jnp.int32), pltpu.SemaphoreType.DMA((3,))],
        source=pltpu.HBM,
    )(off, vel, occ)
    zr = shifted(z, "gz", -1)
    low, high = (jnp.concatenate([part, zr[None]]) for part in (v[0:6], v[18:24]))
    from_ym, from_yp = both_sides(low, high, "gy")
    m = call(widen_kernel, f32(37, *tile))(v, zr, from_ym, from_yp)
    from_xm = shifted(m, "gx", 1)
    from_xp = shifted(m, "gx", -1)
    d0, r0, z0, acc0 = call(
        own_column_kernel,
        (f32(12, *tile), f32(18, *tile), f32(*tile), f32(16, *tile)),
        [vmem(36, *tile), vmem(18, *tile), vmem(18, *tile)],
    )(m, ownx, theta)
    sizes = tuple(lax.axis_size(axis) for axis in AXES)
    devices = sizes[0] * sizes[1] * sizes[2]
    here = jnp.reshape(lax.axis_index(AXES).astype(jnp.int32), (1,))
    d, rm, rp, tally = call(
        functools.partial(side_columns_kernel, sizes),
        (f32(12, *tile), f32(18, *tile), f32(18, *tile), f32(devices, LANES)),
        [vmem(36, *tile)] * 2 + [vmem(18, *tile)] * 4 + [vmem(16, *tile)],
        scalars=1,
    )(here, m, ownx, theta, from_xm, from_xp, d0, z0, acc0)
    s = r0 + shifted(rp, "gx", 1) + shifted(rm, "gx", -1)
    back_ym, back_yp = both_sides(s[0:3], s[15:18], "gy")
    tallies = lax.all_to_all(tally, AXES, 0, 0, tiled=True)
    force, stress, level = call(
        functools.partial(finish_kernel, float(ROWS * LANES * devices)),
        tuple(jax.ShapeDtypeStruct(x, jnp.float32) for x in (off.shape, (3, 3), (1, 1))),
    )(d, s, back_ym, back_yp, tallies)
    return force.reshape(offset.shape), stress, level.reshape(1)


def solution(mesh):
    spec = P(None, None, *AXES)
    return jax.shard_map(
        per_device,
        mesh=mesh,
        in_specs=(spec, spec, P(*AXES), P(None, None, None, *AXES)),
        out_specs=(spec, P(), P()),
        check_vma=False,
    )
```

```python
import functools

import jax
import jax.numpy as jnp
from jax import lax
from jax.experimental import pallas as pl
from jax.experimental.pallas import tpu as pltpu
from jax.sharding import PartitionSpec as P


AXES = ("gx", "gy", "gz")
ROWS = 4
LANES = 128
SLOTS = 8
FAR = 100.0
NOISE_SCALE = 15.0
REST = 25.0 / 15.0
DRAG = 4.5 / 15.0
HALF_ROOT = 0.7071067811865476
BACK = 16


def tile_index(dx, dy, dz):
    if dz == 1:
        return 5 + (dy + 1) * 3 + (dx + 1)
    return {(0, 0): 0, (1, 0): 1, (-1, 1): 2, (0, 1): 3, (1, 1): 4}[(dx, dy)]


COLUMN_TILES = {
    0: [(0, 0), (1, 0), (-1, 1), (0, 1), (1, 1)],
    1: [(0, 0), (1, 0), (-1, 1), (0, 1), (1, 1)],
    -1: [(1, 0), (-1, 1), (0, 1), (1, 1)],
}
PRODUCTS = [(0, 0), (0, 1), (0, 2), (1, 1), (1, 2), (2, 2)]


def lane_iota():
    return lax.broadcasted_iota(jnp.int32, (SLOTS, LANES), 1)


def slot_iota():
    return lax.broadcasted_iota(jnp.int32, (SLOTS, LANES), 0)


def row_of(ref, *index):
    *lead, s = index
    return jnp.broadcast_to(ref[(*lead, pl.ds(s, 1), slice(None))], (SLOTS, LANES))


def pack_kernel(off_hbm, vel_hbm, occ_hbm, v_ref, ownx_ref, z_ref, off_ref, vel_ref, occ_ref, sems):
    copies = [
        pltpu.make_async_copy(src, dst, sems.at[i])
        for i, (src, dst) in enumerate([(off_hbm, off_ref), (vel_hbm, vel_ref), (occ_hbm, occ_ref)])
    ]
    for copy in copies:
        copy.start()
    for copy in copies:
        copy.wait()
    lane = lane_iota()
    slot = slot_iota()
    z = jnp.zeros((SLOTS, LANES), jnp.float32)
    for y in range(ROWS):
        live = slot < jnp.broadcast_to(occ_ref[pl.ds(y, 1), :], (SLOTS, LANES))
        for c in range(6):
            if c < 3:
                val = off_ref[c, pl.ds(y, SLOTS, stride=ROWS), :]
                if c == 0:
                    ownx_ref[y] = jnp.where(live, val, FAR)
                    val = jnp.where(live, val, -FAR)
            else:
                val = vel_ref[c - 3, pl.ds(y, SLOTS, stride=ROWS), :] * DRAG
            v_ref[y * 6 + c] = val
            at = (y + 1) * 6 + c
            z = jnp.where(lane == at, pltpu.roll(val, at, 1), z)
    z_ref[...] = z


def convert_kernel(noise_ref, th_ref):
    @pl.loop(0, th_ref.shape[0] // 256)
    def _(i):
        at = pl.ds(pl.multiple_of(i * 256, 256), 256)
        th_ref[at, :] = noise_ref[at, :].astype(jnp.float32)


def widen_kernel(v_ref, zr_ref, ym_ref, yp_ref, m_ref):
    lane = lane_iota()
    for c in range(6):
        m_ref[c] = ym_ref[c]
        m_ref[30 + c] = yp_ref[c]
        for y in range(ROWS):
            m_ref[(y + 1) * 6 + c] = v_ref[y * 6 + c]
    z = jnp.where(lane < 6, pltpu.roll(ym_ref[6], LANES - 24, 1), zr_ref[...])
    z = jnp.where((lane >= 30) & (lane < 36), pltpu.roll(yp_ref[6], 24, 1), z)
    m_ref[36] = z


def next_plane(m_ref, up_ref):
    lane = lane_iota()
    z = m_ref[36]
    for row in range(6):
        for c in range(6):
            at = row * 6 + c
            val = pltpu.roll(m_ref[at], LANES - 1, 1)
            val = jnp.where(lane == LANES - 1, pltpu.roll(z, LANES - 1 - at, 1), val)
            if c == 2:
                val = val + 1.0
            up_ref[at] = val


def row_pairs(y, columns, own_ref, ownx_ref, th_ref, rl_refs, ru_refs, vir):
    slot = slot_iota()
    d = [[None] * 3 for _ in range(SLOTS)]
    for dx, level_ref, up_ref in columns:
        for dy, dz in COLUMN_TILES[dx]:
            k = tile_index(dx, dy, dz)
            src = up_ref if dz else level_ref
            base = (y + 1 + dy) * 6
            oth = [src[base + c] for c in range(6)]
            if dx:
                oth[0] = oth[0] + float(dx)
            if dy:
                oth[1] = oth[1] + float(dy)
            r = [None] * 3
            for s in range(SLOTS):
                if k == 0 and s == SLOTS - 1:
                    continue
                own = [row_of(ownx_ref, y, s)] + [row_of(own_ref, (y + 1) * 6 + c, s) for c in range(1, 6)]
                sep = [own[a] - oth[a] for a in range(3)]
                rel = [own[3 + a] - oth[3 + a] for a in range(3)]
                dist2 = sep[0] * sep[0] + sep[1] * sep[1] + sep[2] * sep[2]
                u = jnp.maximum(lax.rsqrt(dist2) - 1.0, 0.0)
                dot = sep[0] * rel[0] + sep[1] * rel[1] + sep[2] * rel[2]
                theta = th_ref[pl.ds(k * 256 + s * 32 + y, SLOTS, stride=ROWS), :]
                if k == 0:
                    theta = (theta + th_ref[pl.ds(s * ROWS + y, SLOTS, stride=32), :]) * HALF_ROOT
                fr = u * ((theta + REST) - u * dot)
                if k == 0:
                    fr = jnp.where(slot > s, fr, 0.0)
                for a in range(3):
                    f = fr * sep[a]
                    d[s][a] = f if d[s][a] is None else d[s][a] + f
                    r[a] = f if r[a] is None else r[a] + f
            ref = (ru_refs if dz else rl_refs)[dx]
            at = (y + 1 + dy) * 3
            for a in range(3):
                ref[at + a] = ref[at + a] + r[a]
            vir = [t - oth[a] * r[b] for t, (a, b) in zip(vir, PRODUCTS)]
    for s in range(SLOTS):
        own = [row_of(ownx_ref, y, s)] + [row_of(own_ref, (y + 1) * 6 + c, s) for c in range(1, 3)]
        vir = [t + own[a] * d[s][b] for t, (a, b) in zip(vir, PRODUCTS)]
    return d, vir


def settle(rl_ref, ru_ref, out_ref):
    lane = lane_iota()
    z = jnp.zeros((SLOTS, LANES), jnp.float32)
    for at in range(18):
        up = ru_ref[at]
        z = jnp.where(lane == at, pltpu.roll(up, at + 1, 1), z)
        out_ref[at] = rl_ref[at] + jnp.where(lane == 0, 0.0, pltpu.roll(up, 1, 1))
    return z


def send_past(z, sizes, at, dx, tally, rows_ref):
    lane = lax.broadcasted_iota(jnp.int32, (1, LANES), 1)
    column = (at[0] + (dx + sizes[0])) % sizes[0] * sizes[1]
    for dy, row, count, place in [(-1, 0, 1, 3), (0, 1, 4, 0), (1, 5, 1, 0)]:
        line = tally
        for t in range(SLOTS):
            to = BACK + t * 12 + place * 3
            moved = pltpu.roll(z[t : t + 1, :], (to - row * 3) % LANES, 1)
            line = jnp.where((lane >= to) & (lane < to + 3 * count), moved, line)
        dest = (column + (at[1] + (dy + sizes[1])) % sizes[1]) * sizes[2] + (at[2] + 1) % sizes[2]
        rows_ref[pl.ds(dest, 1), :] = line


def own_column_kernel(m_ref, ownx_ref, th_ref, d_ref, r_ref, z_ref, acc_ref, up_ref, rl_ref, ru_ref):
    next_plane(m_ref, up_ref)
    zero = jnp.zeros((18, SLOTS, LANES), jnp.float32)
    rl_ref[...] = zero
    ru_ref[...] = zero
    acc_ref[...] = jnp.zeros((16, SLOTS, LANES), jnp.float32)

    @pl.loop(0, ROWS)
    def _(y):
        vir = [acc_ref[i] for i in range(6)]
        d, vir = row_pairs(y, [(0, m_ref, up_ref)], m_ref, ownx_ref, th_ref, {0: rl_ref}, {0: ru_ref}, vir)
        for i in range(6):
            acc_ref[i] = vir[i]
        for s in range(SLOTS):
            for a in range(3):
                part = d[s][a]
                d_ref[y * 3 + a, pl.ds(s, 1), :] = jnp.sum(part, axis=0, keepdims=True)
        base = (y + 1) * 6
        live = jnp.where(m_ref[base] > -0.5 * FAR, 1.0, 0.0)
        vel = [m_ref[base + 3 + a] for a in range(3)]
        for i, (a, b) in enumerate(PRODUCTS):
            acc_ref[6 + i] = acc_ref[6 + i] + live * vel[a] * vel[b]
        acc_ref[12] = acc_ref[12] + live

    z_ref[...] = settle(rl_ref, ru_ref, r_ref)


def side_columns_kernel(
    sizes, here_ref, m_ref, ownx_ref, th_ref, xm_ref, xp_ref, d0_ref, z0_ref, acc0_ref,
    d_ref, rm_ref, rp_ref, tally_ref,
    um_ref, up_ref, rlm_ref, rum_ref, rlp_ref, rup_ref, acc_ref,
):
    next_plane(xm_ref, um_ref)
    next_plane(xp_ref, up_ref)
    zero = jnp.zeros((18, SLOTS, LANES), jnp.float32)
    for ref in (rlm_ref, rum_ref, rlp_ref, rup_ref):
        ref[...] = zero
    acc_ref[...] = acc0_ref[...]

    @pl.loop(0, ROWS)
    def _(y):
        vir = [acc_ref[i] for i in range(6)]
        d, vir = row_pairs(
            y, [(1, xp_ref, up_ref), (-1, xm_ref, um_ref)], m_ref, ownx_ref, th_ref,
            {1: rlp_ref, -1: rlm_ref}, {1: rup_ref, -1: rum_ref}, vir,
        )
        for i in range(6):
            acc_ref[i] = vir[i]
        for s in range(SLOTS):
            for a in range(3):
                at = (y * 3 + a, pl.ds(s, 1), slice(None))
                d_ref[at] = d0_ref[at] + jnp.sum(d[s][a], axis=0, keepdims=True)

    planes = [settle(rlm_ref, rum_ref, rm_ref), z0_ref[...], settle(rlp_ref, rup_ref, rp_ref)]
    acc = [acc_ref[i] for i in range(13)]
    sums = [NOISE_SCALE * acc[i] + acc[6 + i] * (1.0 / (DRAG * DRAG)) for i in range(6)]
    lines = [sums[PRODUCTS.index((min(a, b), max(a, b)))] for a in range(3) for b in range(3)]
    lines += [(acc[6] + acc[9] + acc[11]) * (1.0 / (DRAG * DRAG)), acc[12]]
    lane = lax.broadcasted_iota(jnp.int32, (16, LANES), 1)
    line = lax.broadcasted_iota(jnp.int32, (16, LANES), 0)
    lines = [jnp.sum(x, axis=0, keepdims=True) for x in lines]
    held = jnp.concatenate(lines + [jnp.zeros((16 - len(lines), LANES), jnp.float32)], axis=0)
    held = jnp.where(lane == line, jnp.sum(held, axis=1, keepdims=True), 0.0)
    tally = jnp.sum(held, axis=0, keepdims=True)
    tally_ref[...] = jnp.broadcast_to(tally, tally_ref.shape)
    at = (here_ref[0] // (sizes[1] * sizes[2]), here_ref[0] // sizes[2] % sizes[1], here_ref[0] % sizes[2])
    for dx, z in zip((-1, 0, 1), planes):
        send_past(z, sizes, at, dx, tally, tally_ref)


def finish_kernel(cells, d_ref, s_ref, ym_ref, yp_ref, tallies_ref, f_ref, stress_ref, level_ref):
    lane = lane_iota()
    slot = slot_iota()
    total = jnp.broadcast_to(jnp.sum(tallies_ref[...], axis=0, keepdims=True), (SLOTS, LANES))
    stress = jnp.where(slot == 1, pltpu.roll(total, LANES - 3, 1), total)
    stress = jnp.where(slot == 2, pltpu.roll(total, LANES - 6, 1), stress) * (1.0 / cells)
    stress_ref[...] = stress[0:3, 0:3]
    level = pltpu.roll(total, LANES - 9, 1) / (3.0 * pltpu.roll(total, LANES - 10, 1) - 3.0)
    level_ref[...] = level[0:1, 0:1]
    z = pltpu.roll(total, LANES - BACK, 1)
    for t in range(1, SLOTS):
        z = jnp.where(slot == t, pltpu.roll(total, LANES - BACK - t * 12, 1), z)
    for y in range(ROWS):
        for a in range(3):
            at = (y + 1) * 3 + a
            back = s_ref[at]
            if y == 0:
                back = back + ym_ref[a]
            if y == ROWS - 1:
                back = back + yp_ref[a]
            back = back + jnp.where(lane == 0, pltpu.roll(z, (LANES - y * 3 - a) % LANES, 1), 0.0)
            f_ref[a, pl.ds(y, SLOTS, stride=ROWS), :] = NOISE_SCALE * (d_ref[y * 3 + a] - back)


def f32(*shape):
    return pltpu.VMEM(shape, jnp.float32)


def vmem(*shape):
    return pltpu.VMEM(shape, jnp.float32)


def call(kernel, out_shape, scratch=(), source=None, scalars=0):
    space = pl.BlockSpec(memory_space=pltpu.VMEM)

    def run(*args):
        specs = [pl.BlockSpec(memory_space=source or pltpu.VMEM) for _ in args]
        specs[:scalars] = [pl.BlockSpec(memory_space=pltpu.SMEM)] * scalars
        if source is not pltpu.VMEM:
            held = [pltpu.with_memory_space_constraint(a, source or pltpu.VMEM) for a in args[scalars:]]
            args = (*args[:scalars], *held)
        return pl.pallas_call(
            kernel,
            out_shape=out_shape,
            in_specs=specs,
            out_specs=jax.tree.map(lambda _: space, out_shape),
            scratch_shapes=list(scratch),
            compiler_params=pltpu.CompilerParams(vmem_limit_bytes=16 << 20),
        )(*args)

    return run


def swapped(shard, axis, first):
    count = lax.axis_size(axis)
    pairs = [((first + i) % count, (first + i + 1) % count) for i in range(0, count, 2)]
    return lax.ppermute(shard, axis, pairs + [(j, i) for i, j in pairs])


def both_sides(low, high, axis):
    even = lax.axis_index(axis) % 2 == 0
    outer = swapped(jnp.where(even, low, high), axis, 1)
    inner = swapped(jnp.where(even, high, low), axis, 0)
    return jnp.where(even, outer, inner), jnp.where(even, inner, outer)


def shifted(shard, axis, by):
    count = lax.axis_size(axis)
    return lax.ppermute(shard, axis, [(i, (i + by) % count) for i in range(count)])


def per_device(offset, velocity, occupancy, noise):
    off = offset.reshape(3, SLOTS * ROWS, LANES)
    vel = velocity.reshape(3, SLOTS * ROWS, LANES)
    occ = occupancy.reshape(ROWS, LANES)
    tile = (SLOTS, LANES)
    lines = 14 * SLOTS * SLOTS * ROWS
    theta = call(convert_kernel, f32(lines, LANES), source=pltpu.VMEM)(noise.reshape(lines, LANES))
    v, ownx, z = call(
        pack_kernel,
        (f32(24, *tile), f32(ROWS, *tile), f32(*tile)),
        [vmem(*off.shape), vmem(*off.shape), pltpu.VMEM(occ.shape, jnp.int32), pltpu.SemaphoreType.DMA((3,))],
        source=pltpu.HBM,
    )(off, vel, occ)
    zr = shifted(z, "gz", -1)
    low, high = (jnp.concatenate([part, zr[None]]) for part in (v[0:6], v[18:24]))
    from_ym, from_yp = both_sides(low, high, "gy")
    m = call(widen_kernel, f32(37, *tile))(v, zr, from_ym, from_yp)
    from_xm = shifted(m, "gx", 1)
    from_xp = shifted(m, "gx", -1)
    d0, r0, z0, acc0 = call(
        own_column_kernel,
        (f32(12, *tile), f32(18, *tile), f32(*tile), f32(16, *tile)),
        [vmem(36, *tile), vmem(18, *tile), vmem(18, *tile)],
    )(m, ownx, theta)
    sizes = tuple(lax.axis_size(axis) for axis in AXES)
    devices = sizes[0] * sizes[1] * sizes[2]
    here = jnp.reshape(lax.axis_index(AXES).astype(jnp.int32), (1,))
    d, rm, rp, tally = call(
        functools.partial(side_columns_kernel, sizes),
        (f32(12, *tile), f32(18, *tile), f32(18, *tile), f32(devices, LANES)),
        [vmem(36, *tile)] * 2 + [vmem(18, *tile)] * 4 + [vmem(16, *tile)],
        scalars=1,
    )(here, m, ownx, theta, from_xm, from_xp, d0, z0, acc0)
    s = r0 + shifted(rp, "gx", 1) + shifted(rm, "gx", -1)
    back_ym, back_yp = both_sides(s[0:3], s[15:18], "gy")
    tallies = lax.all_to_all(tally, AXES, 0, 0, tiled=True)
    force, stress, level = call(
        functools.partial(finish_kernel, float(ROWS * LANES * devices)),
        tuple(jax.ShapeDtypeStruct(x, jnp.float32) for x in (off.shape, (3, 3), (1, 1))),
    )(d, s, back_ym, back_yp, tallies)
    return force.reshape(offset.shape), stress, level.reshape(1)


def solution(mesh):
    spec = P(None, None, *AXES)
    return jax.shard_map(
        per_device,
        mesh=mesh,
        in_specs=(spec, spec, P(*AXES), P(None, None, None, *AXES)),
        out_specs=(spec, P(), P()),
        check_vma=False,
    )
```

```python
import functools

import jax
import jax.numpy as jnp
from jax import lax
from jax.experimental import pallas as pl
from jax.experimental.pallas import tpu as pltpu
from jax.sharding import PartitionSpec as P


AXES = ("gx", "gy", "gz")
ROWS = 4
LANES = 128
SLOTS = 8
FAR = 100.0
NOISE_SCALE = 15.0
REST = 25.0 / 15.0
DRAG = 4.5 / 15.0
HALF_ROOT = 0.7071067811865476
BACK = 16


def tile_index(dx, dy, dz):
    if dz == 1:
        return 5 + (dy + 1) * 3 + (dx + 1)
    return 3 + dx if dy else dx * dx


TILES = [(0, 0), (1, 0), (-1, 1), (0, 1), (1, 1)]
PRODUCTS = [(0, 0), (0, 1), (0, 2), (1, 1), (1, 2), (2, 2)]


def lane_iota():
    return lax.broadcasted_iota(jnp.int32, (SLOTS, LANES), 1)


def slot_iota():
    return lax.broadcasted_iota(jnp.int32, (SLOTS, LANES), 0)


def row_of(ref, *index):
    *lead, s = index
    return jnp.broadcast_to(ref[(*lead, pl.ds(s, 1), slice(None))], (SLOTS, LANES))


def pack_kernel(off_hbm, vel_hbm, occ_hbm, v_ref, ownx_ref, z_ref, off_ref, vel_ref, occ_ref, sems):
    copies = [
        pltpu.make_async_copy(src, dst, sems.at[i])
        for i, (src, dst) in enumerate([(off_hbm, off_ref), (vel_hbm, vel_ref), (occ_hbm, occ_ref)])
    ]
    for copy in copies:
        copy.start()
    for copy in copies:
        copy.wait()
    lane = lane_iota()
    slot = slot_iota()
    z = jnp.zeros((SLOTS, LANES), jnp.float32)
    for y in range(ROWS):
        live = slot < jnp.broadcast_to(occ_ref[pl.ds(y, 1), :], (SLOTS, LANES))
        for c in range(6):
            if c < 3:
                val = off_ref[c, pl.ds(y, SLOTS, stride=ROWS), :]
                if c == 0:
                    ownx_ref[y] = jnp.where(live, val, FAR)
                    val = jnp.where(live, val, -FAR)
            else:
                val = vel_ref[c - 3, pl.ds(y, SLOTS, stride=ROWS), :] * DRAG
            v_ref[y * 6 + c] = val
            at = (y + 1) * 6 + c
            z = jnp.where(lane == at, pltpu.roll(val, at, 1), z)
    z_ref[...] = z


def convert_kernel(noise_ref, th_ref, ready_ref):
    ready_ref[...] = jnp.zeros_like(ready_ref)

    @pl.loop(0, th_ref.shape[0] // 256)
    def _(i):
        at = pl.ds(pl.multiple_of(i * 256, 256), 256)
        th_ref[at, :] = noise_ref[at, :].astype(jnp.float32)


def widen_kernel(v_ref, zr_ref, ym_ref, yp_ref, ready_ref, m_ref):
    lane = lane_iota()
    for c in range(6):
        m_ref[c] = ym_ref[c]
        m_ref[30 + c] = yp_ref[c]
        for y in range(ROWS):
            m_ref[(y + 1) * 6 + c] = v_ref[y * 6 + c]
    z = jnp.where(lane < 6, pltpu.roll(ym_ref[6], LANES - 24, 1), zr_ref[...])
    z = jnp.where((lane >= 30) & (lane < 36), pltpu.roll(yp_ref[6], 24, 1), z)
    m_ref[36] = z


def next_plane(m_ref, up_ref):
    lane = lane_iota()
    z = m_ref[36]
    for row in range(6):
        for c in range(6):
            at = row * 6 + c
            val = pltpu.roll(m_ref[at], LANES - 1, 1)
            val = jnp.where(lane == LANES - 1, pltpu.roll(z, LANES - 1 - at, 1), val)
            if c == 2:
                val = val + 1.0
            up_ref[at] = val


def row_pairs(y, dx, level_ref, up_ref, own_ref, ownx_ref, th_ref, rl_ref, ru_ref, vir):
    slot = slot_iota()
    own_column = isinstance(dx, int)
    d = [[None] * 3 for _ in range(SLOTS)]
    for dy, dz in TILES:
        k = tile_index(dx, dy, dz)
        src = up_ref if dz else level_ref
        base = (y + 1 + dy) * 6
        oth = [src[base + c] for c in range(6)]
        if not own_column:
            step = dx.astype(jnp.float32)
            if (dy, dz) == (0, 0):
                step = jnp.where(dx == 1, step, -2.0 * FAR)
            oth[0] = oth[0] + step
        if dy:
            oth[1] = oth[1] + float(dy)
        self_tile = own_column and (dy, dz) == (0, 0)
        r = [None] * 3
        for s in range(SLOTS):
            if self_tile and s == SLOTS - 1:
                continue
            own = [row_of(ownx_ref, y, s)] + [row_of(own_ref, (y + 1) * 6 + c, s) for c in range(1, 6)]
            sep = [own[a] - oth[a] for a in range(3)]
            rel = [own[3 + a] - oth[3 + a] for a in range(3)]
            dist2 = sep[0] * sep[0] + sep[1] * sep[1] + sep[2] * sep[2]
            u = jnp.maximum(lax.rsqrt(dist2) - 1.0, 0.0)
            dot = sep[0] * rel[0] + sep[1] * rel[1] + sep[2] * rel[2]
            theta = th_ref[pl.ds(k * 256 + s * 32 + y, SLOTS, stride=ROWS), :]
            if self_tile:
                theta = (theta + th_ref[pl.ds(s * ROWS + y, SLOTS, stride=32), :]) * HALF_ROOT
            fr = u * ((theta + REST) - u * dot)
            if self_tile:
                fr = jnp.where(slot > s, fr, 0.0)
            for a in range(3):
                f = fr * sep[a]
                d[s][a] = f if d[s][a] is None else d[s][a] + f
                r[a] = f if r[a] is None else r[a] + f
        ref = ru_ref if dz else rl_ref
        at = (y + 1 + dy) * 3
        for a in range(3):
            ref[at + a] = ref[at + a] + r[a]
        vir = [t - oth[a] * r[b] for t, (a, b) in zip(vir, PRODUCTS)]
    for s in range(SLOTS):
        own = [row_of(ownx_ref, y, s)] + [row_of(own_ref, (y + 1) * 6 + c, s) for c in range(1, 3)]
        vir = [t + own[a] * d[s][b] for t, (a, b) in zip(vir, PRODUCTS)]
    return d, vir


def settle(rl_ref, ru_ref, out_ref):
    lane = lane_iota()
    z = jnp.zeros((SLOTS, LANES), jnp.float32)
    for at in range(18):
        up = ru_ref[at]
        z = jnp.where(lane == at, pltpu.roll(up, at + 1, 1), z)
        out_ref[at] = rl_ref[at] + jnp.where(lane == 0, 0.0, pltpu.roll(up, 1, 1))
    return z


def send_past(z, sizes, at, dx, tally, rows_ref):
    lane = lax.broadcasted_iota(jnp.int32, (1, LANES), 1)
    column = (at[0] + (dx + sizes[0])) % sizes[0] * sizes[1]
    for dy, row, count, place in [(-1, 0, 1, 3), (0, 1, 4, 0), (1, 5, 1, 0)]:
        line = tally
        for t in range(SLOTS):
            to = BACK + t * 12 + place * 3
            moved = pltpu.roll(z[t : t + 1, :], (to - row * 3) % LANES, 1)
            line = jnp.where((lane >= to) & (lane < to + 3 * count), moved, line)
        dest = (column + (at[1] + (dy + sizes[1])) % sizes[1]) * sizes[2] + (at[2] + 1) % sizes[2]
        rows_ref[pl.ds(dest, 1), :] = line


def own_column_kernel(m_ref, ownx_ref, th_ref, d_ref, r_ref, z_ref, acc_ref, up_ref, rl_ref, ru_ref):
    next_plane(m_ref, up_ref)
    zero = jnp.zeros((18, SLOTS, LANES), jnp.float32)
    rl_ref[...] = zero
    ru_ref[...] = zero
    acc_ref[...] = jnp.zeros((16, SLOTS, LANES), jnp.float32)

    @pl.loop(0, ROWS)
    def _(y):
        vir = [acc_ref[i] for i in range(6)]
        d, vir = row_pairs(y, 0, m_ref, up_ref, m_ref, ownx_ref, th_ref, rl_ref, ru_ref, vir)
        for i in range(6):
            acc_ref[i] = vir[i]
        for s in range(SLOTS):
            for a in range(3):
                part = d[s][a]
                d_ref[y * 3 + a, pl.ds(s, 1), :] = jnp.sum(part, axis=0, keepdims=True)
        base = (y + 1) * 6
        live = jnp.where(m_ref[base] > -0.5 * FAR, 1.0, 0.0)
        vel = [m_ref[base + 3 + a] for a in range(3)]
        for i, (a, b) in enumerate(PRODUCTS):
            acc_ref[6 + i] = acc_ref[6 + i] + live * vel[a] * vel[b]
        acc_ref[12] = acc_ref[12] + live

    z_ref[...] = settle(rl_ref, ru_ref, r_ref)


def side_column(dx, m_ref, ownx_ref, th_ref, x_ref, d_in_ref, acc_in_ref, d_ref, r_ref, acc_ref, up_ref, rl_ref, ru_ref):
    next_plane(x_ref, up_ref)
    zero = jnp.zeros((18, SLOTS, LANES), jnp.float32)
    rl_ref[...] = zero
    ru_ref[...] = zero
    acc_ref[...] = acc_in_ref[...]

    @pl.loop(0, ROWS)
    def _(y):
        vir = [acc_ref[i] for i in range(6)]
        d, vir = row_pairs(y, dx, x_ref, up_ref, m_ref, ownx_ref, th_ref, rl_ref, ru_ref, vir)
        for i in range(6):
            acc_ref[i] = vir[i]
        for s in range(SLOTS):
            for a in range(3):
                at = (y * 3 + a, pl.ds(s, 1), slice(None))
                d_ref[at] = d_in_ref[at] + jnp.sum(d[s][a], axis=0, keepdims=True)

    return settle(rl_ref, ru_ref, r_ref)


def near_column_kernel(
    here_ref, m_ref, ownx_ref, th_ref, x_ref, d0_ref, acc0_ref, d_ref, r_ref, z_ref, acc_ref, *scratch
):
    dx = 1 - 2 * (here_ref[0] % 2)
    z_ref[...] = side_column(dx, m_ref, ownx_ref, th_ref, x_ref, d0_ref, acc0_ref, d_ref, r_ref, acc_ref, *scratch)


def far_column_kernel(
    sizes, here_ref, m_ref, ownx_ref, th_ref, x_ref, d0_ref, acc0_ref, z0_ref, z1_ref,
    d_ref, r_ref, tally_ref, acc_ref, *scratch,
):
    dx = 2 * (here_ref[0] % 2) - 1
    z = side_column(dx, m_ref, ownx_ref, th_ref, x_ref, d0_ref, acc0_ref, d_ref, r_ref, acc_ref, *scratch)
    planes = [(0, z0_ref[...]), (-dx, z1_ref[...]), (dx, z)]
    acc = [acc_ref[i] for i in range(13)]
    sums = [NOISE_SCALE * acc[i] + acc[6 + i] * (1.0 / (DRAG * DRAG)) for i in range(6)]
    lines = [sums[PRODUCTS.index((min(a, b), max(a, b)))] for a in range(3) for b in range(3)]
    lines += [(acc[6] + acc[9] + acc[11]) * (1.0 / (DRAG * DRAG)), acc[12]]
    lane = lax.broadcasted_iota(jnp.int32, (16, LANES), 1)
    line = lax.broadcasted_iota(jnp.int32, (16, LANES), 0)
    lines = [jnp.sum(x, axis=0, keepdims=True) for x in lines]
    held = jnp.concatenate(lines + [jnp.zeros((16 - len(lines), LANES), jnp.float32)], axis=0)
    held = jnp.where(lane == line, jnp.sum(held, axis=1, keepdims=True), 0.0)
    tally = jnp.sum(held, axis=0, keepdims=True)
    tally_ref[...] = jnp.broadcast_to(tally, tally_ref.shape)
    at = [here_ref[i] for i in range(3)]
    for step, z in planes:
        send_past(z, sizes, at, step, tally, tally_ref)


def finish_kernel(cells, d_ref, s_ref, ym_ref, yp_ref, tallies_ref, f_ref, stress_ref, level_ref):
    lane = lane_iota()
    slot = slot_iota()
    total = jnp.broadcast_to(jnp.sum(tallies_ref[...], axis=0, keepdims=True), (SLOTS, LANES))
    stress = jnp.where(slot == 1, pltpu.roll(total, LANES - 3, 1), total)
    stress = jnp.where(slot == 2, pltpu.roll(total, LANES - 6, 1), stress) * (1.0 / cells)
    stress_ref[...] = stress[0:3, 0:3]
    level = pltpu.roll(total, LANES - 9, 1) / (3.0 * pltpu.roll(total, LANES - 10, 1) - 3.0)
    level_ref[...] = level[0:1, 0:1]
    z = pltpu.roll(total, LANES - BACK, 1)
    for t in range(1, SLOTS):
        z = jnp.where(slot == t, pltpu.roll(total, LANES - BACK - t * 12, 1), z)
    for y in range(ROWS):
        for a in range(3):
            at = (y + 1) * 3 + a
            back = s_ref[at]
            if y == 0:
                back = back + ym_ref[a]
            if y == ROWS - 1:
                back = back + yp_ref[a]
            back = back + jnp.where(lane == 0, pltpu.roll(z, (LANES - y * 3 - a) % LANES, 1), 0.0)
            f_ref[a, pl.ds(y, SLOTS, stride=ROWS), :] = NOISE_SCALE * (d_ref[y * 3 + a] - back)


def f32(*shape):
    return pltpu.VMEM(shape, jnp.float32)


def vmem(*shape):
    return pltpu.VMEM(shape, jnp.float32)


def call(kernel, out_shape, scratch=(), source=None, scalars=0):
    space = pl.BlockSpec(memory_space=pltpu.VMEM)

    def run(*args):
        specs = [pl.BlockSpec(memory_space=source or pltpu.VMEM) for _ in args]
        specs[:scalars] = [pl.BlockSpec(memory_space=pltpu.SMEM)] * scalars
        if source is not pltpu.VMEM:
            held = [pltpu.with_memory_space_constraint(a, source or pltpu.VMEM) for a in args[scalars:]]
            args = (*args[:scalars], *held)
        return pl.pallas_call(
            kernel,
            out_shape=out_shape,
            in_specs=specs,
            out_specs=jax.tree.map(lambda _: space, out_shape),
            scratch_shapes=list(scratch),
            compiler_params=pltpu.CompilerParams(vmem_limit_bytes=16 << 20),
        )(*args)

    return run


def swapped(shard, axis, first):
    count = lax.axis_size(axis)
    pairs = [((first + i) % count, (first + i + 1) % count) for i in range(0, count, 2)]
    return lax.ppermute(shard, axis, pairs + [(j, i) for i, j in pairs])


def both_sides(low, high, axis):
    even = lax.axis_index(axis) % 2 == 0
    outer = swapped(jnp.where(even, low, high), axis, 1)
    inner = swapped(jnp.where(even, high, low), axis, 0)
    return jnp.where(even, outer, inner), jnp.where(even, inner, outer)


def shifted(shard, axis, by):
    count = lax.axis_size(axis)
    return lax.ppermute(shard, axis, [(i, (i + by) % count) for i in range(count)])


def per_device(offset, velocity, occupancy, noise):
    off = offset.reshape(3, SLOTS * ROWS, LANES)
    vel = velocity.reshape(3, SLOTS * ROWS, LANES)
    occ = occupancy.reshape(ROWS, LANES)
    tile = (SLOTS, LANES)
    lines = 14 * SLOTS * SLOTS * ROWS
    theta, ready = call(convert_kernel, (f32(lines, LANES), f32(*tile)), source=pltpu.VMEM)(noise.reshape(lines, LANES))
    v, ownx, z = call(
        pack_kernel,
        (f32(24, *tile), f32(ROWS, *tile), f32(*tile)),
        [vmem(*off.shape), vmem(*off.shape), pltpu.VMEM(occ.shape, jnp.int32), pltpu.SemaphoreType.DMA((3,))],
        source=pltpu.HBM,
    )(off, vel, occ)
    zr = shifted(z, "gz", -1)
    low, high = (jnp.concatenate([part, zr[None]]) for part in (v[0:6], v[18:24]))
    from_ym, from_yp = both_sides(low, high, "gy")
    m = call(widen_kernel, f32(37, *tile))(v, zr, from_ym, from_yp, ready)
    far = swapped(m, "gx", 1)
    near = swapped(m, "gx", 0)
    d0, r0, z0, acc0 = call(
        own_column_kernel,
        (f32(12, *tile), f32(18, *tile), f32(*tile), f32(16, *tile)),
        [vmem(36, *tile), vmem(18, *tile), vmem(18, *tile)],
    )(m, ownx, theta)
    sizes = tuple(lax.axis_size(axis) for axis in AXES)
    devices = sizes[0] * sizes[1] * sizes[2]
    here = jnp.stack([lax.axis_index(axis).astype(jnp.int32) for axis in AXES])
    scratch = [vmem(36, *tile), vmem(18, *tile), vmem(18, *tile)]
    d1, r1, z1, acc1 = call(
        near_column_kernel,
        (f32(12, *tile), f32(18, *tile), f32(*tile), f32(16, *tile)),
        scratch,
        scalars=1,
    )(here, m, ownx, theta, near, d0, acc0)
    d, r2, tally = call(
        functools.partial(far_column_kernel, sizes),
        (f32(12, *tile), f32(18, *tile), f32(devices, LANES)),
        [vmem(16, *tile), *scratch],
        scalars=1,
    )(here, m, ownx, theta, far, d1, acc1, z0, z1)
    s = r0 + swapped(r2, "gx", 1) + swapped(r1, "gx", 0)
    back_ym, back_yp = both_sides(s[0:3], s[15:18], "gy")
    tallies = lax.all_to_all(tally, AXES, 0, 0, tiled=True)
    force, stress, level = call(
        functools.partial(finish_kernel, float(ROWS * LANES * devices)),
        tuple(jax.ShapeDtypeStruct(x, jnp.float32) for x in (off.shape, (3, 3), (1, 1))),
    )(d, s, back_ym, back_yp, tallies)
    return force.reshape(offset.shape), stress, level.reshape(1)


def solution(mesh):
    spec = P(None, None, *AXES)
    return jax.shard_map(
        per_device,
        mesh=mesh,
        in_specs=(spec, spec, P(*AXES), P(None, None, None, *AXES)),
        out_specs=(spec, P(), P()),
        check_vma=False,
    )
```

```python
import functools

import jax
import jax.numpy as jnp
from jax import lax
from jax.experimental import pallas as pl
from jax.experimental.pallas import tpu as pltpu
from jax.sharding import PartitionSpec as P


AXES = ("gx", "gy", "gz")
ROWS = 4
LANES = 128
SLOTS = 8
FAR = 100.0
NOISE_SCALE = 15.0
REST = 25.0 / 15.0
DRAG = 4.5 / 15.0
HALF_ROOT = 0.7071067811865476
BACK = 16


def tile_index(dx, dy, dz):
    if dz == 1:
        return 5 + (dy + 1) * 3 + (dx + 1)
    return 3 + dx if dy else dx * dx


TILES = [(0, 0), (1, 0), (-1, 1), (0, 1), (1, 1)]
PRODUCTS = [(0, 0), (0, 1), (0, 2), (1, 1), (1, 2), (2, 2)]


def lane_iota():
    return lax.broadcasted_iota(jnp.int32, (SLOTS, LANES), 1)


def slot_iota():
    return lax.broadcasted_iota(jnp.int32, (SLOTS, LANES), 0)


def row_of(ref, *index):
    *lead, s = index
    return jnp.broadcast_to(ref[(*lead, pl.ds(s, 1), slice(None))], (SLOTS, LANES))


def pack_kernel(off_hbm, vel_hbm, occ_hbm, v_ref, ownx_ref, z_ref, off_ref, vel_ref, occ_ref, sems):
    copies = [
        pltpu.make_async_copy(src, dst, sems.at[i])
        for i, (src, dst) in enumerate([(off_hbm, off_ref), (vel_hbm, vel_ref), (occ_hbm, occ_ref)])
    ]
    for copy in copies:
        copy.start()
    for copy in copies:
        copy.wait()
    lane = lane_iota()
    slot = slot_iota()
    z = jnp.zeros((SLOTS, LANES), jnp.float32)
    for y in range(ROWS):
        live = slot < jnp.broadcast_to(occ_ref[pl.ds(y, 1), :], (SLOTS, LANES))
        for c in range(6):
            if c < 3:
                val = off_ref[c, pl.ds(y, SLOTS, stride=ROWS), :]
                if c == 0:
                    ownx_ref[y] = jnp.where(live, val, FAR)
                    val = jnp.where(live, val, -FAR)
            else:
                val = vel_ref[c - 3, pl.ds(y, SLOTS, stride=ROWS), :] * DRAG
            v_ref[y * 6 + c] = val
            at = (y + 1) * 6 + c
            z = jnp.where(lane == at, pltpu.roll(val, at, 1), z)
    z_ref[...] = z


def convert_kernel(noise_ref, th_ref, ready_ref):
    ready_ref[...] = jnp.zeros_like(ready_ref)

    @pl.loop(0, th_ref.shape[0] // 256)
    def _(i):
        at = pl.ds(pl.multiple_of(i * 256, 256), 256)
        th_ref[at, :] = noise_ref[at, :].astype(jnp.float32)


def widen_kernel(v_ref, zr_ref, ym_ref, yp_ref, ready_ref, m_ref):
    lane = lane_iota()
    for c in range(6):
        m_ref[c] = ym_ref[c]
        m_ref[30 + c] = yp_ref[c]
        for y in range(ROWS):
            m_ref[(y + 1) * 6 + c] = v_ref[y * 6 + c]
    z = jnp.where(lane < 6, pltpu.roll(ym_ref[6], LANES - 24, 1), zr_ref[...])
    z = jnp.where((lane >= 30) & (lane < 36), pltpu.roll(yp_ref[6], 24, 1), z)
    m_ref[36] = z


def next_plane(m_ref, up_ref):
    lane = lane_iota()
    z = m_ref[36]
    for row in range(6):
        for c in range(6):
            at = row * 6 + c
            val = pltpu.roll(m_ref[at], LANES - 1, 1)
            val = jnp.where(lane == LANES - 1, pltpu.roll(z, LANES - 1 - at, 1), val)
            if c == 2:
                val = val + 1.0
            up_ref[at] = val


def row_pairs(y, dx, tiles, level_ref, up_ref, own_ref, ownx_ref, th_ref, rl_ref, ru_ref, vir):
    slot = slot_iota()
    own_column = isinstance(dx, int)
    d = [[None] * 3 for _ in range(SLOTS)]
    for dy, dz in tiles:
        k = tile_index(dx, dy, dz)
        src = up_ref if dz else level_ref
        base = (y + 1 + dy) * 6
        oth = [src[base + c] for c in range(6)]
        if not own_column:
            oth[0] = oth[0] + dx.astype(jnp.float32)
        if dy:
            oth[1] = oth[1] + float(dy)
        self_tile = own_column and (dy, dz) == (0, 0)
        r = [None] * 3
        for s in range(SLOTS):
            if self_tile and s == SLOTS - 1:
                continue
            own = [row_of(ownx_ref, y, s)] + [row_of(own_ref, (y + 1) * 6 + c, s) for c in range(1, 6)]
            sep = [own[a] - oth[a] for a in range(3)]
            rel = [own[3 + a] - oth[3 + a] for a in range(3)]
            dist2 = sep[0] * sep[0] + sep[1] * sep[1] + sep[2] * sep[2]
            u = jnp.maximum(lax.rsqrt(dist2) - 1.0, 0.0)
            dot = sep[0] * rel[0] + sep[1] * rel[1] + sep[2] * rel[2]
            theta = th_ref[pl.ds(k * 256 + s * 32 + y, SLOTS, stride=ROWS), :]
            if self_tile:
                theta = (theta + th_ref[pl.ds(s * ROWS + y, SLOTS, stride=32), :]) * HALF_ROOT
            fr = u * ((theta + REST) - u * dot)
            if self_tile:
                fr = jnp.where(slot > s, fr, 0.0)
            for a in range(3):
                f = fr * sep[a]
                d[s][a] = f if d[s][a] is None else d[s][a] + f
                r[a] = f if r[a] is None else r[a] + f
        ref = ru_ref if dz else rl_ref
        at = (y + 1 + dy) * 3
        for a in range(3):
            ref[at + a] = ref[at + a] + r[a]
        vir = [t - oth[a] * r[b] for t, (a, b) in zip(vir, PRODUCTS)]
    for s in range(SLOTS):
        own = [row_of(ownx_ref, y, s)] + [row_of(own_ref, (y + 1) * 6 + c, s) for c in range(1, 3)]
        vir = [t + own[a] * d[s][b] for t, (a, b) in zip(vir, PRODUCTS)]
    return d, vir


def settle(rl_ref, ru_ref, out_ref):
    lane = lane_iota()
    z = jnp.zeros((SLOTS, LANES), jnp.float32)
    for at in range(18):
        up = ru_ref[at]
        z = jnp.where(lane == at, pltpu.roll(up, at + 1, 1), z)
        out_ref[at] = rl_ref[at] + jnp.where(lane == 0, 0.0, pltpu.roll(up, 1, 1))
    return z


def send_past(z, sizes, at, dx, tally, rows_ref):
    lane = lax.broadcasted_iota(jnp.int32, (1, LANES), 1)
    column = (at[0] + (dx + sizes[0])) % sizes[0] * sizes[1]
    for dy, row, count, place in [(-1, 0, 1, 3), (0, 1, 4, 0), (1, 5, 1, 0)]:
        line = tally
        for t in range(SLOTS):
            to = BACK + t * 12 + place * 3
            moved = pltpu.roll(z[t : t + 1, :], (to - row * 3) % LANES, 1)
            line = jnp.where((lane >= to) & (lane < to + 3 * count), moved, line)
        dest = (column + (at[1] + (dy + sizes[1])) % sizes[1]) * sizes[2] + (at[2] + 1) % sizes[2]
        rows_ref[pl.ds(dest, 1), :] = line


def own_column_kernel(m_ref, ownx_ref, th_ref, d_ref, r_ref, z_ref, acc_ref, up_ref, rl_ref, ru_ref):
    next_plane(m_ref, up_ref)
    zero = jnp.zeros((18, SLOTS, LANES), jnp.float32)
    rl_ref[...] = zero
    ru_ref[...] = zero
    acc_ref[...] = jnp.zeros((16, SLOTS, LANES), jnp.float32)

    @pl.loop(0, ROWS)
    def _(y):
        vir = [acc_ref[i] for i in range(6)]
        d, vir = row_pairs(y, 0, TILES, m_ref, up_ref, m_ref, ownx_ref, th_ref, rl_ref, ru_ref, vir)
        for i in range(6):
            acc_ref[i] = vir[i]
        for s in range(SLOTS):
            for a in range(3):
                part = d[s][a]
                d_ref[y * 3 + a, pl.ds(s, 1), :] = jnp.sum(part, axis=0, keepdims=True)
        base = (y + 1) * 6
        live = jnp.where(m_ref[base] > -0.5 * FAR, 1.0, 0.0)
        vel = [m_ref[base + 3 + a] for a in range(3)]
        for i, (a, b) in enumerate(PRODUCTS):
            acc_ref[6 + i] = acc_ref[6 + i] + live * vel[a] * vel[b]
        acc_ref[12] = acc_ref[12] + live

    z_ref[...] = settle(rl_ref, ru_ref, r_ref)


def side_column(dx, m_ref, ownx_ref, th_ref, x_ref, d_in_ref, acc_in_ref, d_ref, r_ref, acc_ref, up_ref, rl_ref, ru_ref):
    next_plane(x_ref, up_ref)
    zero = jnp.zeros((18, SLOTS, LANES), jnp.float32)
    rl_ref[...] = zero
    ru_ref[...] = zero
    acc_ref[...] = acc_in_ref[...]

    def pairs(tiles, from_ref):
        @pl.loop(0, ROWS)
        def _(y):
            vir = [acc_ref[i] for i in range(6)]
            d, vir = row_pairs(y, dx, tiles, x_ref, up_ref, m_ref, ownx_ref, th_ref, rl_ref, ru_ref, vir)
            for i in range(6):
                acc_ref[i] = vir[i]
            for s in range(SLOTS):
                for a in range(3):
                    at = (y * 3 + a, pl.ds(s, 1), slice(None))
                    d_ref[at] = from_ref[at] + jnp.sum(d[s][a], axis=0, keepdims=True)

    pairs(TILES[1:], d_in_ref)

    @pl.when(dx == 1)
    def _():
        pairs(TILES[:1], d_ref)

    return settle(rl_ref, ru_ref, r_ref)


def near_column_kernel(
    m_ref, ownx_ref, th_ref, x_ref, d0_ref, acc0_ref, d_ref, r_ref, z_ref, acc_ref, *scratch
):
    dx = 1 - 2 * (lax.axis_index("gx") % 2)
    z_ref[...] = side_column(dx, m_ref, ownx_ref, th_ref, x_ref, d0_ref, acc0_ref, d_ref, r_ref, acc_ref, *scratch)


def far_column_kernel(
    sizes, m_ref, ownx_ref, th_ref, x_ref, d0_ref, acc0_ref, z0_ref, z1_ref,
    d_ref, r_ref, tally_ref, acc_ref, *scratch,
):
    dx = 2 * (lax.axis_index("gx") % 2) - 1
    z = side_column(dx, m_ref, ownx_ref, th_ref, x_ref, d0_ref, acc0_ref, d_ref, r_ref, acc_ref, *scratch)
    planes = [(0, z0_ref[...]), (-dx, z1_ref[...]), (dx, z)]
    acc = [acc_ref[i] for i in range(13)]
    sums = [NOISE_SCALE * acc[i] + acc[6 + i] * (1.0 / (DRAG * DRAG)) for i in range(6)]
    lines = [sums[PRODUCTS.index((min(a, b), max(a, b)))] for a in range(3) for b in range(3)]
    lines += [(acc[6] + acc[9] + acc[11]) * (1.0 / (DRAG * DRAG)), acc[12]]
    lane = lax.broadcasted_iota(jnp.int32, (16, LANES), 1)
    line = lax.broadcasted_iota(jnp.int32, (16, LANES), 0)
    lines = [jnp.sum(x, axis=0, keepdims=True) for x in lines]
    held = jnp.concatenate(lines + [jnp.zeros((16 - len(lines), LANES), jnp.float32)], axis=0)
    held = jnp.where(lane == line, jnp.sum(held, axis=1, keepdims=True), 0.0)
    tally = jnp.sum(held, axis=0, keepdims=True)
    tally_ref[...] = jnp.broadcast_to(tally, tally_ref.shape)
    at = [lax.axis_index(axis) for axis in AXES]
    for step, z in planes:
        send_past(z, sizes, at, step, tally, tally_ref)


def finish_kernel(cells, d_ref, s_ref, ym_ref, yp_ref, tallies_ref, f_ref, stress_ref, level_ref):
    lane = lane_iota()
    slot = slot_iota()
    total = jnp.broadcast_to(jnp.sum(tallies_ref[...], axis=0, keepdims=True), (SLOTS, LANES))
    stress = jnp.where(slot == 1, pltpu.roll(total, LANES - 3, 1), total)
    stress = jnp.where(slot == 2, pltpu.roll(total, LANES - 6, 1), stress) * (1.0 / cells)
    stress_ref[...] = stress[0:3, 0:3]
    level = pltpu.roll(total, LANES - 9, 1) / (3.0 * pltpu.roll(total, LANES - 10, 1) - 3.0)
    level_ref[...] = level[0:1, 0:1]
    z = pltpu.roll(total, LANES - BACK, 1)
    for t in range(1, SLOTS):
        z = jnp.where(slot == t, pltpu.roll(total, LANES - BACK - t * 12, 1), z)
    for y in range(ROWS):
        for a in range(3):
            at = (y + 1) * 3 + a
            back = s_ref[at]
            if y == 0:
                back = back + ym_ref[a]
            if y == ROWS - 1:
                back = back + yp_ref[a]
            back = back + jnp.where(lane == 0, pltpu.roll(z, (LANES - y * 3 - a) % LANES, 1), 0.0)
            f_ref[a, pl.ds(y, SLOTS, stride=ROWS), :] = NOISE_SCALE * (d_ref[y * 3 + a] - back)


def f32(*shape):
    return pltpu.VMEM(shape, jnp.float32)


def vmem(*shape):
    return pltpu.VMEM(shape, jnp.float32)


def call(kernel, out_shape, scratch=(), source=None):
    space = pl.BlockSpec(memory_space=pltpu.VMEM)

    def run(*args):
        if source is not pltpu.VMEM:
            args = [pltpu.with_memory_space_constraint(a, source or pltpu.VMEM) for a in args]
        return pl.pallas_call(
            kernel,
            out_shape=out_shape,
            in_specs=[pl.BlockSpec(memory_space=source or pltpu.VMEM) for _ in args],
            out_specs=jax.tree.map(lambda _: space, out_shape),
            scratch_shapes=list(scratch),
            compiler_params=pltpu.CompilerParams(vmem_limit_bytes=16 << 20),
        )(*args)

    return run


def swapped(shard, axis, first):
    count = lax.axis_size(axis)
    pairs = [((first + i) % count, (first + i + 1) % count) for i in range(0, count, 2)]
    return lax.ppermute(shard, axis, pairs + [(j, i) for i, j in pairs])


def both_sides(low, high, axis):
    even = lax.axis_index(axis) % 2 == 0
    outer = swapped(jnp.where(even, low, high), axis, 1)
    inner = swapped(jnp.where(even, high, low), axis, 0)
    return jnp.where(even, outer, inner), jnp.where(even, inner, outer)


def shifted(shard, axis, by):
    count = lax.axis_size(axis)
    return lax.ppermute(shard, axis, [(i, (i + by) % count) for i in range(count)])


def per_device(offset, velocity, occupancy, noise):
    off = offset.reshape(3, SLOTS * ROWS, LANES)
    vel = velocity.reshape(3, SLOTS * ROWS, LANES)
    occ = occupancy.reshape(ROWS, LANES)
    tile = (SLOTS, LANES)
    lines = 14 * SLOTS * SLOTS * ROWS
    theta, ready = call(convert_kernel, (f32(lines, LANES), f32(*tile)), source=pltpu.VMEM)(noise.reshape(lines, LANES))
    v, ownx, z = call(
        pack_kernel,
        (f32(24, *tile), f32(ROWS, *tile), f32(*tile)),
        [vmem(*off.shape), vmem(*off.shape), pltpu.VMEM(occ.shape, jnp.int32), pltpu.SemaphoreType.DMA((3,))],
        source=pltpu.HBM,
    )(off, vel, occ)
    zr = shifted(z, "gz", -1)
    low, high = (jnp.concatenate([part, zr[None]]) for part in (v[0:6], v[18:24]))
    from_ym, from_yp = both_sides(low, high, "gy")
    m = call(widen_kernel, f32(37, *tile))(v, zr, from_ym, from_yp, ready)
    far = swapped(m, "gx", 1)
    near = swapped(m, "gx", 0)
    d0, r0, z0, acc0 = call(
        own_column_kernel,
        (f32(12, *tile), f32(18, *tile), f32(*tile), f32(16, *tile)),
        [vmem(36, *tile), vmem(18, *tile), vmem(18, *tile)],
    )(m, ownx, theta)
    sizes = tuple(lax.axis_size(axis) for axis in AXES)
    devices = sizes[0] * sizes[1] * sizes[2]
    scratch = [vmem(36, *tile), vmem(18, *tile), vmem(18, *tile)]
    d1, r1, z1, acc1 = call(
        near_column_kernel,
        (f32(12, *tile), f32(18, *tile), f32(*tile), f32(16, *tile)),
        scratch,
    )(m, ownx, theta, near, d0, acc0)
    d, r2, tally = call(
        functools.partial(far_column_kernel, sizes),
        (f32(12, *tile), f32(18, *tile), f32(devices, LANES)),
        [vmem(16, *tile), *scratch],
    )(m, ownx, theta, far, d1, acc1, z0, z1)
    s = r0 + swapped(r2, "gx", 1) + swapped(r1, "gx", 0)
    back_ym, back_yp = both_sides(s[0:3], s[15:18], "gy")
    tallies = lax.all_to_all(tally, AXES, 0, 0, tiled=True)
    force, stress, level = call(
        functools.partial(finish_kernel, float(ROWS * LANES * devices)),
        tuple(jax.ShapeDtypeStruct(x, jnp.float32) for x in (off.shape, (3, 3), (1, 1))),
    )(d, s, back_ym, back_yp, tallies)
    return force.reshape(offset.shape), stress, level.reshape(1)


def solution(mesh):
    spec = P(None, None, *AXES)
    return jax.shard_map(
        per_device,
        mesh=mesh,
        in_specs=(spec, spec, P(*AXES), P(None, None, None, *AXES)),
        out_specs=(spec, P(), P()),
        check_vma=False,
    )
```

```python
import functools

import jax
import jax.numpy as jnp
from jax import lax
from jax.experimental import pallas as pl
from jax.experimental.pallas import tpu as pltpu
from jax.sharding import PartitionSpec as P


AXES = ("gx", "gy", "gz")
ROWS = 4
LANES = 128
SLOTS = 8
FAR = 100.0
NOISE_SCALE = 15.0
REST = 25.0 / 15.0
DRAG = 4.5 / 15.0
HALF_ROOT = 0.7071067811865476
BACK = 16


def tile_index(dx, dy, dz):
    if dz == 1:
        return 5 + (dy + 1) * 3 + (dx + 1)
    return 3 + dx if dy else dx * dx


TILES = [(0, 0), (1, 0), (-1, 1), (0, 1), (1, 1)]
PRODUCTS = [(0, 0), (0, 1), (0, 2), (1, 1), (1, 2), (2, 2)]


def lane_iota():
    return lax.broadcasted_iota(jnp.int32, (SLOTS, LANES), 1)


def slot_iota():
    return lax.broadcasted_iota(jnp.int32, (SLOTS, LANES), 0)


def row_of(ref, *index):
    *lead, s = index
    return jnp.broadcast_to(ref[(*lead, pl.ds(s, 1), slice(None))], (SLOTS, LANES))


def pack_kernel(off_hbm, vel_hbm, occ_hbm, v_ref, ownx_ref, z_ref, off_ref, vel_ref, occ_ref, sems):
    copies = [
        pltpu.make_async_copy(src, dst, sems.at[i])
        for i, (src, dst) in enumerate([(off_hbm, off_ref), (vel_hbm, vel_ref), (occ_hbm, occ_ref)])
    ]
    for copy in copies:
        copy.start()
    for copy in copies:
        copy.wait()
    lane = lane_iota()
    slot = slot_iota()
    z = jnp.zeros((SLOTS, LANES), jnp.float32)
    for y in range(ROWS):
        live = slot < jnp.broadcast_to(occ_ref[pl.ds(y, 1), :], (SLOTS, LANES))
        for c in range(6):
            if c < 3:
                val = off_ref[c, pl.ds(y, SLOTS, stride=ROWS), :]
                if c == 0:
                    ownx_ref[y] = jnp.where(live, val, FAR)
                    val = jnp.where(live, val, -FAR)
            else:
                val = vel_ref[c - 3, pl.ds(y, SLOTS, stride=ROWS), :] * DRAG
            v_ref[y * 6 + c] = val
            at = (y + 1) * 6 + c
            z = jnp.where(lane == at, pltpu.roll(val, at, 1), z)
    z_ref[...] = z


def convert_kernel(noise_ref, th_ref, ready_ref):
    ready_ref[...] = jnp.zeros_like(ready_ref)

    @pl.loop(0, th_ref.shape[0] // 256)
    def _(i):
        at = pl.ds(pl.multiple_of(i * 256, 256), 256)
        th_ref[at, :] = noise_ref[at, :].astype(jnp.float32) + REST


def widen_kernel(v_ref, zr_ref, ym_ref, yp_ref, ready_ref, m_ref):
    lane = lane_iota()
    for c in range(6):
        m_ref[c] = ym_ref[c]
        m_ref[30 + c] = yp_ref[c]
        for y in range(ROWS):
            m_ref[(y + 1) * 6 + c] = v_ref[y * 6 + c]
    z = jnp.where(lane < 6, pltpu.roll(ym_ref[6], LANES - 24, 1), zr_ref[...])
    z = jnp.where((lane >= 30) & (lane < 36), pltpu.roll(yp_ref[6], 24, 1), z)
    m_ref[36] = z


def next_plane(m_ref, up_ref):
    lane = lane_iota()
    z = m_ref[36]
    for row in range(6):
        for c in range(6):
            at = row * 6 + c
            val = pltpu.roll(m_ref[at], LANES - 1, 1)
            val = jnp.where(lane == LANES - 1, pltpu.roll(z, LANES - 1 - at, 1), val)
            if c == 2:
                val = val + 1.0
            up_ref[at] = val


def row_pairs(y, dx, tiles, level_ref, up_ref, own_ref, ownx_ref, th_ref, rl_ref, ru_ref, vir):
    slot = slot_iota()
    own_column = isinstance(dx, int)
    d = [[None] * 3 for _ in range(SLOTS)]
    for dy, dz in tiles:
        k = tile_index(dx, dy, dz)
        src = up_ref if dz else level_ref
        base = (y + 1 + dy) * 6
        oth = [src[base + c] for c in range(6)]
        if not own_column:
            oth[0] = oth[0] + dx.astype(jnp.float32)
        if dy:
            oth[1] = oth[1] + float(dy)
        self_tile = own_column and (dy, dz) == (0, 0)
        r = [None] * 3
        for s in range(SLOTS):
            if self_tile and s == SLOTS - 1:
                continue
            own = [row_of(ownx_ref, y, s)] + [row_of(own_ref, (y + 1) * 6 + c, s) for c in range(1, 6)]
            sep = [own[a] - oth[a] for a in range(3)]
            rel = [own[3 + a] - oth[3 + a] for a in range(3)]
            dist2 = sep[0] * sep[0] + sep[1] * sep[1] + sep[2] * sep[2]
            u = jnp.maximum(lax.rsqrt(dist2) - 1.0, 0.0)
            dot = sep[0] * rel[0] + sep[1] * rel[1] + sep[2] * rel[2]
            theta = th_ref[pl.ds(k * 256 + s * 32 + y, SLOTS, stride=ROWS), :]
            if self_tile:
                theta = (theta + th_ref[pl.ds(s * ROWS + y, SLOTS, stride=32), :]) * HALF_ROOT + REST * (1.0 - 2.0 * HALF_ROOT)
            fr = u * (theta - u * dot)
            if self_tile:
                fr = jnp.where(slot > s, fr, 0.0)
            for a in range(3):
                f = fr * sep[a]
                d[s][a] = f if d[s][a] is None else d[s][a] + f
                r[a] = f if r[a] is None else r[a] + f
        ref = ru_ref if dz else rl_ref
        at = (y + 1 + dy) * 3
        for a in range(3):
            ref[at + a] = ref[at + a] + r[a]
        vir = [t - oth[a] * r[b] for t, (a, b) in zip(vir, PRODUCTS)]
    for s in range(SLOTS):
        own = [row_of(ownx_ref, y, s)] + [row_of(own_ref, (y + 1) * 6 + c, s) for c in range(1, 3)]
        vir = [t + own[a] * d[s][b] for t, (a, b) in zip(vir, PRODUCTS)]
    return d, vir


def settle(rl_ref, ru_ref, out_ref):
    lane = lane_iota()
    z = jnp.zeros((SLOTS, LANES), jnp.float32)
    for at in range(18):
        up = ru_ref[at]
        z = jnp.where(lane == at, pltpu.roll(up, at + 1, 1), z)
        out_ref[at] = rl_ref[at] + jnp.where(lane == 0, 0.0, pltpu.roll(up, 1, 1))
    return z


def send_past(z, sizes, at, dx, tally, rows_ref):
    lane = lax.broadcasted_iota(jnp.int32, (1, LANES), 1)
    column = (at[0] + (dx + sizes[0])) % sizes[0] * sizes[1]
    for dy, row, count, place in [(-1, 0, 1, 3), (0, 1, 4, 0), (1, 5, 1, 0)]:
        line = tally
        for t in range(SLOTS):
            to = BACK + t * 12 + place * 3
            moved = pltpu.roll(z[t : t + 1, :], (to - row * 3) % LANES, 1)
            line = jnp.where((lane >= to) & (lane < to + 3 * count), moved, line)
        dest = (column + (at[1] + (dy + sizes[1])) % sizes[1]) * sizes[2] + (at[2] + 1) % sizes[2]
        rows_ref[pl.ds(dest, 1), :] = line


def own_column_kernel(m_ref, ownx_ref, th_ref, d_ref, r_ref, z_ref, acc_ref, up_ref, rl_ref, ru_ref):
    next_plane(m_ref, up_ref)
    zero = jnp.zeros((18, SLOTS, LANES), jnp.float32)
    rl_ref[...] = zero
    ru_ref[...] = zero
    acc_ref[...] = jnp.zeros((16, SLOTS, LANES), jnp.float32)

    @pl.loop(0, ROWS)
    def _(y):
        vir = [acc_ref[i] for i in range(6)]
        d, vir = row_pairs(y, 0, TILES, m_ref, up_ref, m_ref, ownx_ref, th_ref, rl_ref, ru_ref, vir)
        for i in range(6):
            acc_ref[i] = vir[i]
        for s in range(SLOTS):
            for a in range(3):
                part = d[s][a]
                d_ref[y * 3 + a, pl.ds(s, 1), :] = jnp.sum(part, axis=0, keepdims=True)
        base = (y + 1) * 6
        live = jnp.where(m_ref[base] > -0.5 * FAR, 1.0, 0.0)
        vel = [m_ref[base + 3 + a] for a in range(3)]
        for i, (a, b) in enumerate(PRODUCTS):
            acc_ref[6 + i] = acc_ref[6 + i] + live * vel[a] * vel[b]
        acc_ref[12] = acc_ref[12] + live

    z_ref[...] = settle(rl_ref, ru_ref, r_ref)


def side_column(dx, m_ref, ownx_ref, th_ref, x_ref, d_in_ref, acc_in_ref, d_ref, r_ref, acc_ref, up_ref, rl_ref, ru_ref):
    next_plane(x_ref, up_ref)
    zero = jnp.zeros((18, SLOTS, LANES), jnp.float32)
    rl_ref[...] = zero
    ru_ref[...] = zero
    acc_ref[...] = acc_in_ref[...]

    def pairs(tiles, from_ref):
        @pl.loop(0, ROWS)
        def _(y):
            vir = [acc_ref[i] for i in range(6)]
            d, vir = row_pairs(y, dx, tiles, x_ref, up_ref, m_ref, ownx_ref, th_ref, rl_ref, ru_ref, vir)
            for i in range(6):
                acc_ref[i] = vir[i]
            for s in range(SLOTS):
                for a in range(3):
                    at = (y * 3 + a, pl.ds(s, 1), slice(None))
                    d_ref[at] = from_ref[at] + jnp.sum(d[s][a], axis=0, keepdims=True)

    pairs(TILES[1:], d_in_ref)

    @pl.when(dx == 1)
    def _():
        pairs(TILES[:1], d_ref)

    return settle(rl_ref, ru_ref, r_ref)


def near_column_kernel(
    m_ref, ownx_ref, th_ref, x_ref, d0_ref, acc0_ref, d_ref, r_ref, z_ref, acc_ref, *scratch
):
    dx = 1 - 2 * (lax.axis_index("gx") % 2)
    z_ref[...] = side_column(dx, m_ref, ownx_ref, th_ref, x_ref, d0_ref, acc0_ref, d_ref, r_ref, acc_ref, *scratch)


def far_column_kernel(
    sizes, m_ref, ownx_ref, th_ref, x_ref, d0_ref, acc0_ref, z0_ref, z1_ref,
    d_ref, r_ref, tally_ref, acc_ref, *scratch,
):
    dx = 2 * (lax.axis_index("gx") % 2) - 1
    z = side_column(dx, m_ref, ownx_ref, th_ref, x_ref, d0_ref, acc0_ref, d_ref, r_ref, acc_ref, *scratch)
    planes = [(0, z0_ref[...]), (-dx, z1_ref[...]), (dx, z)]
    acc = [acc_ref[i] for i in range(13)]
    sums = [NOISE_SCALE * acc[i] + acc[6 + i] * (1.0 / (DRAG * DRAG)) for i in range(6)]
    lines = [sums[PRODUCTS.index((min(a, b), max(a, b)))] for a in range(3) for b in range(3)]
    lines += [(acc[6] + acc[9] + acc[11]) * (1.0 / (DRAG * DRAG)), acc[12]]
    lane = lax.broadcasted_iota(jnp.int32, (16, LANES), 1)
    line = lax.broadcasted_iota(jnp.int32, (16, LANES), 0)
    lines = [jnp.sum(x, axis=0, keepdims=True) for x in lines]
    held = jnp.concatenate(lines + [jnp.zeros((16 - len(lines), LANES), jnp.float32)], axis=0)
    held = jnp.where(lane == line, jnp.sum(held, axis=1, keepdims=True), 0.0)
    tally = jnp.sum(held, axis=0, keepdims=True)
    tally_ref[...] = jnp.broadcast_to(tally, tally_ref.shape)
    at = [lax.axis_index(axis) for axis in AXES]
    for step, z in planes:
        send_past(z, sizes, at, step, tally, tally_ref)


def finish_kernel(cells, d_ref, s_ref, ym_ref, yp_ref, tallies_ref, f_ref, stress_ref, level_ref):
    lane = lane_iota()
    slot = slot_iota()
    total = jnp.broadcast_to(jnp.sum(tallies_ref[...], axis=0, keepdims=True), (SLOTS, LANES))
    stress = jnp.where(slot == 1, pltpu.roll(total, LANES - 3, 1), total)
    stress = jnp.where(slot == 2, pltpu.roll(total, LANES - 6, 1), stress) * (1.0 / cells)
    stress_ref[...] = stress[0:3, 0:3]
    level = pltpu.roll(total, LANES - 9, 1) / (3.0 * pltpu.roll(total, LANES - 10, 1) - 3.0)
    level_ref[...] = level[0:1, 0:1]
    z = pltpu.roll(total, LANES - BACK, 1)
    for t in range(1, SLOTS):
        z = jnp.where(slot == t, pltpu.roll(total, LANES - BACK - t * 12, 1), z)
    for y in range(ROWS):
        for a in range(3):
            at = (y + 1) * 3 + a
            back = s_ref[at]
            if y == 0:
                back = back + ym_ref[a]
            if y == ROWS - 1:
                back = back + yp_ref[a]
            back = back + jnp.where(lane == 0, pltpu.roll(z, (LANES - y * 3 - a) % LANES, 1), 0.0)
            f_ref[a, pl.ds(y, SLOTS, stride=ROWS), :] = NOISE_SCALE * (d_ref[y * 3 + a] - back)


def f32(*shape):
    return pltpu.VMEM(shape, jnp.float32)


def vmem(*shape):
    return pltpu.VMEM(shape, jnp.float32)


def call(kernel, out_shape, scratch=(), source=None):
    space = pl.BlockSpec(memory_space=pltpu.VMEM)

    def run(*args):
        if source is not pltpu.VMEM:
            args = [pltpu.with_memory_space_constraint(a, source or pltpu.VMEM) for a in args]
        return pl.pallas_call(
            kernel,
            out_shape=out_shape,
            in_specs=[pl.BlockSpec(memory_space=source or pltpu.VMEM) for _ in args],
            out_specs=jax.tree.map(lambda _: space, out_shape),
            scratch_shapes=list(scratch),
            compiler_params=pltpu.CompilerParams(vmem_limit_bytes=16 << 20),
        )(*args)

    return run


def swapped(shard, axis, first):
    count = lax.axis_size(axis)
    pairs = [((first + i) % count, (first + i + 1) % count) for i in range(0, count, 2)]
    return lax.ppermute(shard, axis, pairs + [(j, i) for i, j in pairs])


def both_sides(low, high, axis):
    even = lax.axis_index(axis) % 2 == 0
    outer = swapped(jnp.where(even, low, high), axis, 1)
    inner = swapped(jnp.where(even, high, low), axis, 0)
    return jnp.where(even, outer, inner), jnp.where(even, inner, outer)


def shifted(shard, axis, by):
    count = lax.axis_size(axis)
    return lax.ppermute(shard, axis, [(i, (i + by) % count) for i in range(count)])


def per_device(offset, velocity, occupancy, noise):
    off = offset.reshape(3, SLOTS * ROWS, LANES)
    vel = velocity.reshape(3, SLOTS * ROWS, LANES)
    occ = occupancy.reshape(ROWS, LANES)
    tile = (SLOTS, LANES)
    lines = 14 * SLOTS * SLOTS * ROWS
    theta, ready = call(convert_kernel, (f32(lines, LANES), f32(*tile)), source=pltpu.VMEM)(noise.reshape(lines, LANES))
    v, ownx, z = call(
        pack_kernel,
        (f32(24, *tile), f32(ROWS, *tile), f32(*tile)),
        [vmem(*off.shape), vmem(*off.shape), pltpu.VMEM(occ.shape, jnp.int32), pltpu.SemaphoreType.DMA((3,))],
        source=pltpu.HBM,
    )(off, vel, occ)
    zr = shifted(z, "gz", -1)
    low, high = (jnp.concatenate([part, zr[None]]) for part in (v[0:6], v[18:24]))
    from_ym, from_yp = both_sides(low, high, "gy")
    m = call(widen_kernel, f32(37, *tile))(v, zr, from_ym, from_yp, ready)
    far = swapped(m, "gx", 1)
    near = swapped(m, "gx", 0)
    d0, r0, z0, acc0 = call(
        own_column_kernel,
        (f32(12, *tile), f32(18, *tile), f32(*tile), f32(16, *tile)),
        [vmem(36, *tile), vmem(18, *tile), vmem(18, *tile)],
    )(m, ownx, theta)
    sizes = tuple(lax.axis_size(axis) for axis in AXES)
    devices = sizes[0] * sizes[1] * sizes[2]
    scratch = [vmem(36, *tile), vmem(18, *tile), vmem(18, *tile)]
    d1, r1, z1, acc1 = call(
        near_column_kernel,
        (f32(12, *tile), f32(18, *tile), f32(*tile), f32(16, *tile)),
        scratch,
    )(m, ownx, theta, near, d0, acc0)
    d, r2, tally = call(
        functools.partial(far_column_kernel, sizes),
        (f32(12, *tile), f32(18, *tile), f32(devices, LANES)),
        [vmem(16, *tile), *scratch],
    )(m, ownx, theta, far, d1, acc1, z0, z1)
    s = r0 + swapped(r2, "gx", 1) + swapped(r1, "gx", 0)
    back_ym, back_yp = both_sides(s[0:3], s[15:18], "gy")
    tallies = lax.all_to_all(tally, AXES, 0, 0, tiled=True)
    force, stress, level = call(
        functools.partial(finish_kernel, float(ROWS * LANES * devices)),
        tuple(jax.ShapeDtypeStruct(x, jnp.float32) for x in (off.shape, (3, 3), (1, 1))),
    )(d, s, back_ym, back_yp, tallies)
    return force.reshape(offset.shape), stress, level.reshape(1)


def solution(mesh):
    spec = P(None, None, *AXES)
    return jax.shard_map(
        per_device,
        mesh=mesh,
        in_specs=(spec, spec, P(*AXES), P(None, None, None, *AXES)),
        out_specs=(spec, P(), P()),
        check_vma=False,
    )
```
